16 devices in a mesh: dp: 2 (over z), tp: 8 (over y, x, core).
Axes of the slice: x: 2, y: 2, z: 2, core: 2. Of those that a mesh axis runs over, the one named last changes fastest.
Arguments:
- x_in: bfloat16 [1024, 5120], P('dp'), parts along dimension 0
- lengths: int32 [1024], P('dp'), parts along dimension 0
- norm_gain: bfloat16 [2, 5120], replicated
- w_q: bfloat16 [2, 5120, 5120], P(None, None, 'tp')
- w_k: bfloat16 [2, 5120, 1024], P(None, None, 'tp')
- w_v: bfloat16 [2, 5120, 1024], P(None, None, 'tp')
- w_o: bfloat16 [2, 5120, 5120], P(None, 'tp')
- w_gate: bfloat16 [2, 5120, 13824], P(None, None, 'tp')
- w_up: bfloat16 [2, 5120, 13824], P(None, None, 'tp')
- w_down: bfloat16 [2, 13824, 5120], P(None, 'tp')
- k_cache: bfloat16 [2, 1024, 32, 8, 128], P(None, 'dp', None, 'tp'), parts along dimension 1
- v_cache: bfloat16 [2, 1024, 32, 8, 128], P(None, 'dp', None, 'tp'), parts along dimension 1
Outputs:
- output: bfloat16 [1024, 5120], P('dp'), parts along dimension 0
There are 2 independent parts. The reference program is written for one: setup_inputs(seed, part) draws one part's arguments, and reference() takes and returns one part's arrays. A program takes and returns all parts, laid end to end along the dimension named above; an argument that names none is the same for every part.
All inputs are finite; a program needn't handle non-finite values.
Results may differ from the reference program's by a relative error of at most 0.0174644.
Values are sent between devices in bfloat16 or wider.
A program may use at most 1 GiB of HBM per device.

```python
import math
import jax
import jax.numpy as jnp
from jax import lax

D = 5120
HEADS = 40
KV_HEADS = 8
FF = 13824
HEAD = 128
BATCH = 512
SEQ = 32
LAYERS = 2
ROPE_BASE = 500000
NORM_EPS = 1e-5
GROUP = HEADS // KV_HEADS
LOG_LEVELS = int(math.log2(SEQ)) + 1


def draw_lengths(len_key):
    exp_key, val_key, top_key = jax.random.split(len_key, 3)
    span_exp = jax.random.randint(exp_key, (BATCH,), 0, LOG_LEVELS)
    span_limit = jnp.minimum(jnp.left_shift(jnp.ones_like(span_exp), span_exp), SEQ - 1)
    drawn_len = 1 + jax.random.randint(val_key, (BATCH,), 0, span_limit)
    full_slot = jax.random.randint(top_key, (), 0, BATCH)
    return jnp.where(jnp.arange(BATCH) == full_slot, SEQ - 1, drawn_len).astype(jnp.int32)


def setup_inputs(seed: int = 0, part: int = 0) -> dict:
    base_key = jax.random.key(seed)
    shared_keys = jax.random.split(base_key, 8)
    own_keys = jax.random.split(jax.random.fold_in(base_key, part), 4)
    q_width = HEADS * HEAD
    kv_width = KV_HEADS * HEAD

    def draw_weight(key_index, arr_shape, std_scale):
        return (jax.random.normal(shared_keys[key_index], arr_shape, jnp.float32) * std_scale).astype(jnp.bfloat16)

    return {
        'x_in': jax.random.normal(own_keys[0], (BATCH, D), jnp.float32).astype(jnp.bfloat16),
        'lengths': draw_lengths(own_keys[1]),
        'norm_gain': (1.0 + 0.3 * jax.random.normal(shared_keys[0], (LAYERS, D), jnp.float32)).astype(jnp.bfloat16),
        'w_q': draw_weight(1, (LAYERS, D, q_width), D ** -0.5),
        'w_k': draw_weight(2, (LAYERS, D, kv_width), 2.0 * D ** -0.5),
        'w_v': draw_weight(3, (LAYERS, D, kv_width), D ** -0.5),
        'w_o': draw_weight(4, (LAYERS, q_width, D), 2.0 * q_width ** -0.5),
        'w_gate': draw_weight(5, (LAYERS, D, FF), D ** -0.5),
        'w_up': draw_weight(6, (LAYERS, D, FF), D ** -0.5),
        'w_down': draw_weight(7, (LAYERS, FF, D), FF ** -0.5),
        'k_cache': (2.0 * jax.random.normal(own_keys[2], (LAYERS, BATCH, SEQ, KV_HEADS, HEAD), jnp.float32)).astype(jnp.bfloat16),
        'v_cache': jax.random.normal(own_keys[3], (LAYERS, BATCH, SEQ, KV_HEADS, HEAD), jnp.float32).astype(jnp.bfloat16),
    }


def rms_norm(x_res, gain_row):
    x_f32 = x_res.astype(jnp.float32)
    inv_rms = lax.rsqrt(jnp.mean(x_f32 * x_f32, axis=-1, keepdims=True) + NORM_EPS)
    return (x_f32 * inv_rms * gain_row.astype(jnp.float32)).astype(jnp.bfloat16)


def rope_rotate(head_vecs, positions):
    half_dim = HEAD // 2
    inv_freq = 1.0 / (ROPE_BASE ** (jnp.arange(0, HEAD, 2).astype(jnp.float32) / HEAD))
    angles = positions.astype(jnp.float32)[:, None] * inv_freq[None, :]
    cos_ang = jnp.cos(angles)[:, None, :]
    sin_ang = jnp.sin(angles)[:, None, :]
    vec_f32 = head_vecs.astype(jnp.float32)
    rot_first = vec_f32[..., :half_dim]
    rot_second = vec_f32[..., half_dim:]
    return jnp.concatenate([rot_first * cos_ang - rot_second * sin_ang, rot_second * cos_ang + rot_first * sin_ang], axis=-1).astype(jnp.bfloat16)


def decode_attention(q_rot, k_rot, v_new, k_layer, v_layer, lengths):
    attn_scale = HEAD ** -0.5
    q_f32 = q_rot.astype(jnp.float32)
    cache_logits = jnp.einsum('bkgd,bskd->bkgs', q_f32, k_layer.astype(jnp.float32)) * attn_scale
    valid_mask = jnp.arange(SEQ)[None, :] < lengths[:, None]
    cache_logits = jnp.where(valid_mask[:, None, None, :], cache_logits, -jnp.inf)
    self_logit = jnp.einsum('bkgd,bkd->bkg', q_f32, k_rot.astype(jnp.float32)) * attn_scale
    row_peak = jnp.maximum(jnp.max(cache_logits, axis=-1), self_logit)
    cache_w = jnp.exp(cache_logits - row_peak[..., None])
    self_w = jnp.exp(self_logit - row_peak)
    prob_denom = jnp.sum(cache_w, axis=-1) + self_w
    cache_p = (cache_w / prob_denom[..., None]).astype(jnp.bfloat16)
    self_p = (self_w / prob_denom).astype(jnp.bfloat16)
    cache_part = jnp.einsum('bkgs,bskd->bkgd', cache_p.astype(jnp.float32), v_layer.astype(jnp.float32))
    self_part = self_p.astype(jnp.float32)[..., None] * v_new.astype(jnp.float32)[:, :, None, :]
    return (cache_part + self_part).astype(jnp.bfloat16)


def reference(x_in, lengths, norm_gain, w_q, w_k, w_v, w_o, w_gate, w_up, w_down, k_cache, v_cache):
    def layer_step(x_res, layer_args):
        gain_row, wq_layer, wk_layer, wv_layer, wo_layer, wg_layer, wu_layer, wd_layer, k_layer, v_layer = layer_args
        normed = rms_norm(x_res, gain_row)
        q_proj = jnp.dot(normed, wq_layer, preferred_element_type=jnp.float32).astype(jnp.bfloat16).reshape(BATCH, HEADS, HEAD)
        k_proj = jnp.dot(normed, wk_layer, preferred_element_type=jnp.float32).astype(jnp.bfloat16).reshape(BATCH, KV_HEADS, HEAD)
        v_new = jnp.dot(normed, wv_layer, preferred_element_type=jnp.float32).astype(jnp.bfloat16).reshape(BATCH, KV_HEADS, HEAD)
        q_rot = rope_rotate(q_proj, lengths).reshape(BATCH, KV_HEADS, GROUP, HEAD)
        k_rot = rope_rotate(k_proj, lengths)
        attn_flat = decode_attention(q_rot, k_rot, v_new, k_layer, v_layer, lengths).reshape(BATCH, HEADS * HEAD)
        attn_proj = jnp.dot(attn_flat, wo_layer, preferred_element_type=jnp.float32)
        gate_act = jnp.dot(normed, wg_layer, preferred_element_type=jnp.float32).astype(jnp.bfloat16)
        up_act = jnp.dot(normed, wu_layer, preferred_element_type=jnp.float32).astype(jnp.bfloat16)
        mlp_hidden = (jax.nn.silu(gate_act.astype(jnp.float32)) * up_act.astype(jnp.float32)).astype(jnp.bfloat16)
        mlp_proj = jnp.dot(mlp_hidden, wd_layer, preferred_element_type=jnp.float32)
        x_next = (x_res.astype(jnp.float32) + attn_proj + mlp_proj).astype(jnp.bfloat16)
        return x_next, None

    scan_result = lax.scan(layer_step, x_in, (norm_gain, w_q, w_k, w_v, w_o, w_gate, w_up, w_down, k_cache, v_cache))
    return scan_result[0]
```

```python
import functools

import jax
import jax.numpy as jnp
from jax import lax
from jax.experimental import pallas as pl
from jax.experimental.pallas import tpu as pltpu
from jax.sharding import PartitionSpec as P

NORM_EPS = 1e-5
ROPE_BASE = 500000.0
MESH = pl.DeviceIdType.MESH
BF, F32 = jnp.bfloat16, jnp.float32
NT_DIMS = (((1,), (1,)), ((), ()))


def attend_block(t0, qkv, cos, sin, bound, keys, vals, groups, head, seq):
    rows = pl.ds(t0, 8)
    cached = pl.ds(pl.multiple_of(t0 * seq, 8 * seq), 8 * seq)
    scale = head ** -0.5
    c, s = cos[rows, :], sin[rows, :]
    proj = qkv[rows, :].astype(BF).astype(F32)

    def turn(v):
        return (v * c + pltpu.roll(v, head // 2, 1) * s).astype(BF).astype(F32)

    q = jnp.concatenate([turn(proj[:, head * h:head * (h + 1)]) for h in range(groups)], axis=0)
    k_new = turn(proj[:, groups * head:(groups + 1) * head])
    v_new = proj[:, (groups + 1) * head:]
    logits = lax.dot_general(q.astype(BF), keys[cached, :], NT_DIMS, preferred_element_type=F32) * scale
    logits = logits.reshape(groups, 8, 8 * seq)
    own = jnp.sum(q.reshape(groups, 8, head) * k_new[None], axis=-1, keepdims=True) * scale
    col = lax.broadcasted_iota(jnp.int32, (8, 8 * seq), 1)
    low = lax.broadcasted_iota(jnp.int32, (8, 8 * seq), 0) * seq
    high = jnp.concatenate([bound[rows, :]] * (8 * seq // 128), axis=1) + low
    logits = jnp.where(((col >= low) & (col < high))[None], logits, -jnp.inf)
    peak = jnp.maximum(jnp.max(logits, axis=-1, keepdims=True), own)
    w = jnp.exp(logits - peak)
    w_own = jnp.exp(own - peak)
    inv = 1.0 / (jnp.sum(w, axis=-1, keepdims=True) + w_own)
    p = (w * inv).reshape(groups * 8, 8 * seq).astype(BF)
    p_own = (w_own * inv).astype(BF).astype(F32)
    out = jnp.dot(p, vals[cached, :], preferred_element_type=F32).reshape(groups, 8, head)
    return out + p_own * v_new[None]


def front_kernel(layer, dims, x_hbm, bound, cos, sin, gain, wq, wk, wv, wg, wu, kc, vc, h_ref,
                 x, a, inv_ref, qkv_w, gate_w, up_w, qkv, gate, up, keys, vals, x_sem, w_sem, kv_sem):
    groups, head, seq, kb, steps = dims
    qw = groups * head
    rows, ff = x.shape[0], gate.shape[1]

    def weights(step, slot):
        ks = pl.ds(pl.multiple_of(step * kb, kb), kb)
        pairs = (
            (wq.at[layer, ks, :], qkv_w.at[slot, :, 0:qw]),
            (wk.at[layer, ks, :], qkv_w.at[slot, :, qw:qw + head]),
            (wv.at[layer, ks, :], qkv_w.at[slot, :, qw + head:qw + 2 * head]),
            (wg.at[layer, :, ks], gate_w.at[slot]),
            (wu.at[layer, :, ks], up_w.at[slot]),
        )
        return [pltpu.make_async_copy(s, d, w_sem.at[slot, n]) for n, (s, d) in enumerate(pairs)]

    x_copy = pltpu.make_async_copy(x_hbm, x, x_sem)
    x_copy.start()
    for step in range(2):
        for copy in weights(step, step):
            copy.start()
    k_copy = pltpu.make_async_copy(kc.at[layer], keys, kv_sem.at[0])
    v_copy = pltpu.make_async_copy(vc.at[layer], vals, kv_sem.at[1])
    k_copy.start()
    v_copy.start()
    x_copy.wait()

    @pl.loop(0, rows // 32)
    def _(i):
        r = pl.ds(pl.multiple_of(i * 32, 32), 32)
        total = jnp.zeros((32, 128), F32)
        for c0 in range(0, x.shape[1], 128):
            v = x[r, c0:c0 + 128].astype(F32)
            total = total + v * v
        mean = jnp.sum(total, axis=-1, keepdims=True) / x.shape[1]
        inv_ref[r, :] = jnp.broadcast_to(lax.rsqrt(mean + NORM_EPS), (32, 128))

    @pl.loop(0, steps)
    def _(step):
        slot = lax.rem(step, 2)
        ks = pl.ds(pl.multiple_of(step * kb, kb), kb)
        g = gain[layer:layer + 1, ks]

        @pl.loop(0, rows // 32)
        def _(i):
            r = pl.ds(pl.multiple_of(i * 32, 32), 32)
            a[r, :] = (x[r, ks].astype(F32) * inv_ref[r, 0:1] * g).astype(BF)

        for copy in weights(step, slot):
            copy.wait()
        first = step == 0
        part = lax.dot_general(a[...], gate_w[slot], NT_DIMS, preferred_element_type=F32)
        gate[...] = jnp.where(first, 0.0, gate[...]) + part
        part = lax.dot_general(a[...], up_w[slot], NT_DIMS, preferred_element_type=F32)
        up[...] = jnp.where(first, 0.0, up[...]) + part
        part = jnp.dot(a[...], qkv_w[slot], preferred_element_type=F32)
        qkv[...] = jnp.where(first, 0.0, qkv[...]) + part

        @pl.when(step + 2 < steps)
        def _():
            for copy in weights(step + 2, slot):
                copy.start()

    @pl.loop(0, rows // 16)
    def _(i):
        r = pl.ds(pl.multiple_of(i * 16, 16), 16)
        g16 = gate[r, :].astype(BF).astype(F32)
        u16 = up[r, :].astype(BF).astype(F32)
        h_ref[r, qw:qw + ff] = (g16 * (1.0 / (1.0 + jnp.exp(-g16))) * u16).astype(BF)

    k_copy.wait()
    v_copy.wait()

    @pl.loop(0, rows // 32)
    def _(i):
        for half in range(2):
            t0 = pl.multiple_of(i * 32 + half * 16, 16)
            outs = [attend_block(pl.multiple_of(t0 + 8 * n, 8), qkv, cos, sin, bound, keys, vals, groups, head, seq) for n in range(2)]
            for h in range(groups):
                both = jnp.concatenate([outs[0][h], outs[1][h]], axis=0)
                h_ref[pl.ds(t0, 16), head * h:head * (h + 1)] = both.astype(BF)


def back_kernel(layer, dims, last, h_ref, x_hbm, wo, wd, out_ref, w, send_p, recv_p, own_p, send_i, recv_i, x_own, xg,
                w_sem, x_sem, pair_s, pair_r, ici_s, ici_r, ag_s, ag_r, fwd_s, fwd_r, out_sem):
    cw, qw = dims
    rows, ff = h_ref.shape[0], h_ref.shape[1] - qw
    half = rows // 2
    me = lax.axis_index("tp")
    core, chip = lax.rem(me, 2), me // 2
    mate = me + 1 - 2 * core
    chip_x = chip + 1 - 2 * lax.rem(chip, 2)
    chip_y = chip + 2 - 4 * (chip // 2)
    chip_d = 3 - chip
    order = (chip_d, chip_y, chip_x, chip)

    def cols(device):
        return pl.ds(pl.multiple_of(device * cw, cw), cw)

    def weights(step):
        slot, q = step % 2, order[step]
        copies = []
        for n, device in enumerate((2 * q + 1 - core, 2 * q + core)):
            for m, (src, r0, r1) in enumerate(((wo, 0, qw), (wd, qw, qw + ff))):
                copies.append(pltpu.make_async_copy(
                    src.at[layer, :, cols(device)], w.at[slot, r0:r1, n * cw:(n + 1) * cw], w_sem.at[slot, 2 * n + m]))
        return copies

    for step in range(2):
        for copy in weights(step):
            copy.start()
    x_copy = pltpu.make_async_copy(x_hbm.at[:, cols(me)], x_own, x_sem)
    x_copy.start()

    barrier = pltpu.get_barrier_semaphore()
    for device in (mate, 2 * chip_x + core, 2 * chip_y + core, 2 * chip_d + core):
        pl.semaphore_signal(barrier, inc=1, device_id={"tp": device}, device_id_type=MESH)
    pl.semaphore_wait(barrier, 4)

    def remote(src, dst, s_sem, r_sem, device):
        return pltpu.make_async_remote_copy(src_ref=src, dst_ref=dst, send_sem=s_sem, recv_sem=r_sem,
                                            device_id={"tp": device}, device_id_type=MESH)

    pair = [remote(send_p.at[i], recv_p.at[i], pair_s.at[i], pair_r.at[i], mate) for i in range(4)]
    ici = [remote(send_i.at[i], recv_i.at[i], ici_s.at[i], ici_r.at[i], 2 * order[i] + core) for i in range(3)]

    def settle(i):
        pair[i].wait_recv()
        if i < 3:
            @pl.loop(0, rows // 32)
            def _(n):
                r = pl.ds(pl.multiple_of(n * 32, 32), 32)
                send_i[i, r, :] = (own_p[i, r, :] + recv_p[i, r, :]).astype(BF)
            ici[i].start()

    for step in range(4):
        for copy in weights(step):
            copy.wait()
        part = jnp.dot(h_ref[...], w[step % 2], preferred_element_type=F32)
        send_p[step] = part[:, 0:cw]
        pair[step].start()
        own_p[step] = part[:, cw:2 * cw]
        if step + 2 < 4:
            for copy in weights(step + 2):
                copy.start()
        if step >= 1:
            settle(step - 1)
    settle(3)
    x_copy.wait()
    for i in range(3):
        ici[i].wait_recv()

    @pl.loop(0, rows // 32)
    def _(n):
        r = pl.ds(pl.multiple_of(n * 32, 32), 32)
        total = own_p[3, r, :] + recv_p[3, r, :]
        for i in range(3):
            total = total + recv_i[i, r, :].astype(F32)
        xg[r, cols(me)] = (x_own[r, :].astype(F32) + total).astype(BF)

    def share(r0, r1, owner, s_sem, r_sem, device):
        block = xg.at[r0:r1, cols(owner)]
        return remote(block, block, s_sem, r_sem, device)

    near = [share(0, rows, me, ag_s.at[n], ag_r.at[n], 2 * q + core) for n, q in enumerate((chip_x, chip_y))]
    for copy in near:
        copy.start()
    to_mate = [
        share(0, rows, me, fwd_s.at[0], fwd_r.at[0], mate),
        share(0, rows, 2 * chip_x + core, fwd_s.at[1], fwd_r.at[1], mate),
        share(0, rows, 2 * chip_y + core, fwd_s.at[2], fwd_r.at[2], mate),
        share(0, half, 2 * chip_d + core, fwd_s.at[3], fwd_r.at[3], mate),
        share(half, rows, 2 * chip_d + core, fwd_s.at[4], fwd_r.at[4], mate),
    ]
    far = [
        share(0, half, 2 * chip_x + core, ag_s.at[2], ag_r.at[2], 2 * chip_y + core),
        share(half, rows, 2 * chip_y + core, ag_s.at[3], ag_r.at[3], 2 * chip_x + core),
    ]
    to_mate[0].start()
    for n in range(2):
        near[n].wait_recv()
        far[n].start()
        to_mate[1 + n].start()
    for n in range(2):
        far[n].wait_recv()
        to_mate[3 + n].start()
    for copy in to_mate:
        copy.wait_recv()
    out = pltpu.make_async_copy(xg, out_ref, out_sem)
    out.start()
    for copy in pair + ici + near + far + to_mate:
        copy.wait_send()
    out.wait()


def solution(mesh):
    tp = mesh.shape["tp"]
    arg_specs = (P("dp", None), P("dp"), P(), P(None, None, "tp"), P(None, None, "tp"), P(None, None, "tp"), P(None, "tp", None), P(None, None, "tp"), P(None, None, "tp"), P(None, "tp", None), P(None, "dp", None, "tp", None), P(None, "dp", None, "tp", None))
    hbm = pl.BlockSpec(memory_space=pl.ANY)
    vmem = pl.BlockSpec(memory_space=pltpu.VMEM)
    dma = pltpu.SemaphoreType.DMA

    def per_device(x_in, lengths, norm_gain, w_q, w_k, w_v, w_o, w_gate, w_up, w_down, k_cache, v_cache):
        rows, width = x_in.shape
        layers, _, seq, _, head = k_cache.shape
        qw, ff = w_q.shape[-1], w_gate.shape[-1]
        groups = qw // head
        cw = width // tp
        kb = 2 * cw
        inv_freq = 1.0 / (ROPE_BASE ** (jnp.arange(0, head, 2).astype(F32) / head))
        angles = lengths.astype(F32)[:, None] * inv_freq[None, :]
        cos, sin = jnp.cos(angles), jnp.sin(angles)
        cos = jnp.concatenate([cos, cos], axis=1)
        sin = jnp.concatenate([-sin, sin], axis=1)
        bound = jnp.broadcast_to(lengths[:, None], (rows, 128))
        gain = norm_gain.astype(F32)
        gate_t, up_t = jnp.swapaxes(w_gate, 1, 2), jnp.swapaxes(w_up, 1, 2)
        kc = k_cache.reshape(layers, rows * seq, head)
        vc = v_cache.reshape(layers, rows * seq, head)
        x = x_in
        for layer in range(layers):
            h = pl.pallas_call(
                functools.partial(front_kernel, layer, (groups, head, seq, kb, width // kb)),
                out_shape=jax.ShapeDtypeStruct((rows, qw + ff), BF),
                in_specs=[hbm, vmem, vmem, vmem, vmem] + [hbm] * 7,
                out_specs=vmem,
                scratch_shapes=[
                    pltpu.VMEM((rows, width), BF), pltpu.VMEM((rows, kb), BF), pltpu.VMEM((rows, 128), F32),
                    pltpu.VMEM((2, kb, qw + 2 * head), BF), pltpu.VMEM((2, ff, kb), BF), pltpu.VMEM((2, ff, kb), BF),
                    pltpu.VMEM((rows, qw + 2 * head), F32), pltpu.VMEM((rows, ff), F32), pltpu.VMEM((rows, ff), F32),
                    pltpu.VMEM((rows * seq, head), BF), pltpu.VMEM((rows * seq, head), BF),
                    dma, dma((2, 5)), dma((2,)),
                ],
                compiler_params=pltpu.CompilerParams(vmem_limit_bytes=63 * 2**20),
                name=f"front{layer}",
            )(x, bound, cos, sin, gain, w_q, w_k, w_v, gate_t, up_t, kc, vc)
            x = pl.pallas_call(
                functools.partial(back_kernel, layer, (cw, qw), layer == layers - 1),
                out_shape=jax.ShapeDtypeStruct((rows, width), BF),
                in_specs=[vmem, hbm, hbm, hbm],
                out_specs=hbm,
                scratch_shapes=[
                    pltpu.VMEM((2, qw + ff, kb), BF),
                    pltpu.VMEM((4, rows, cw), F32), pltpu.VMEM((4, rows, cw), F32), pltpu.VMEM((4, rows, cw), F32),
                    pltpu.VMEM((3, rows, cw), BF), pltpu.VMEM((3, rows, cw), BF),
                    pltpu.VMEM((rows, cw), BF), pltpu.VMEM((rows, width), BF),
                    dma((2, 4)), dma, dma((4,)), dma((4,)), dma((3,)), dma((3,)),
                    dma((4,)), dma((4,)), dma((5,)), dma((5,)), dma,
                ],
                compiler_params=pltpu.CompilerParams(vmem_limit_bytes=60 * 2**20, collective_id=layer, has_side_effects=True),
                name=f"back{layer}",
            )(h, x, w_o, w_down)
        return x

    return jax.shard_map(per_device, mesh=mesh, in_specs=arg_specs, out_specs=P("dp", None), check_vma=False)
```

```python
import functools

import jax
import jax.numpy as jnp
from jax import lax
from jax.experimental import pallas as pl
from jax.experimental.pallas import tpu as pltpu
from jax.sharding import PartitionSpec as P

NORM_EPS = 1e-5
ROPE_BASE = 500000.0
MESH = pl.DeviceIdType.MESH
BF, F32 = jnp.bfloat16, jnp.float32
PER = 2
NT_DIMS = (((1,), (1,)), ((), ()))


def attention(qkv, cos, sin, bound, keys, vals, h_ref, bufs, groups, head, seq):
    qb, ob, lb, pb, pob = bufs
    per = qb.shape[1]
    span = 8 * seq
    n_groups = qkv.shape[0] // (8 * per)
    scale = head ** -0.5
    col = lax.broadcasted_iota(jnp.int32, (8, span), 1)
    low = lax.broadcasted_iota(jnp.int32, (8, span), 0) * seq

    def start_of(g, n):
        return pl.multiple_of(g * (8 * per) + 8 * n, 8)

    def project(g):
        slot = lax.rem(g, 2)
        for n in range(per):
            rows = pl.ds(start_of(g, n), 8)
            c, s = cos[rows, :], sin[rows, :]

            def turn(j):
                v = qkv[rows, head * j:head * (j + 1)].astype(BF).astype(F32)
                return (v * c + pltpu.roll(v, head // 2, 1) * s).astype(BF).astype(F32)

            k_new = turn(groups)
            for j in range(groups):
                q = turn(j)
                qb[slot, n, 8 * j:8 * (j + 1), :] = q
                own = jnp.sum(q * k_new, axis=-1, keepdims=True) * scale
                ob[slot, n, 8 * j:8 * (j + 1), :] = jnp.broadcast_to(own, (8, 128))

    def score(g):
        slot = lax.rem(g, 2)
        for n in range(per):
            t0 = start_of(g, n)
            cached = pl.ds(pl.multiple_of(t0 * seq, span), span)
            logits = lax.dot_general(qb[slot, n].astype(BF), keys[cached, :], NT_DIMS, preferred_element_type=F32) * scale
            b = bound[pl.ds(t0, 8), :]
            high = jnp.concatenate([b] * (span // 128), axis=1) + low
            keep = (col >= low) & (col < high)
            for j in range(groups):
                lb[slot, n, 8 * j:8 * (j + 1), :] = jnp.where(keep, logits[8 * j:8 * (j + 1)], -jnp.inf)

    def weigh(g):
        slot = lax.rem(g, 2)
        for n in range(per):
            for j in range(groups):
                r = slice(8 * j, 8 * (j + 1))
                logits, own = lb[slot, n, r, :], ob[slot, n, r, :]
                peak = jnp.maximum(jnp.max(logits, axis=-1, keepdims=True), own)
                w = [jnp.exp(logits[:, c0:c0 + 128] - peak) for c0 in range(0, span, 128)]
                w_own = jnp.exp(own - peak)
                inv = 1.0 / (jnp.sum(sum(w[1:], w[0]), axis=-1, keepdims=True) + w_own)
                for m, v in enumerate(w):
                    pb[slot, n, r, 128 * m:128 * (m + 1)] = v * inv
                pob[slot, n, r, :] = (w_own * inv).astype(BF).astype(F32)

    def mix(g):
        slot = lax.rem(g, 2)
        for n0 in range(0, per, 2):
            outs = []
            for n in (n0, n0 + 1):
                t0 = start_of(g, n)
                cached = pl.ds(pl.multiple_of(t0 * seq, span), span)
                out = jnp.dot(pb[slot, n].astype(BF), vals[cached, :], preferred_element_type=F32)
                v_new = qkv[pl.ds(t0, 8), (groups + 1) * head:].astype(BF).astype(F32)
                outs.append([out[8 * j:8 * (j + 1)] + pob[slot, n, 8 * j:8 * (j + 1), :] * v_new for j in range(groups)])
            for j in range(groups):
                both = jnp.concatenate([outs[0][j], outs[1][j]], axis=0).astype(BF)
                h_ref[pl.ds(pl.multiple_of(start_of(g, n0), 16), 16), head * j:head * (j + 1)] = both

    @pl.loop(0, n_groups + 3)
    def _(i):
        for lag, stage in ((3, mix), (2, weigh), (1, score), (0, project)):
            stage(jnp.clip(i - lag, 0, n_groups - 1))


def place(core, chip, fx, fy):
    x, y = lax.rem(chip, 2), chip // 2
    return 2 * (y + fy * (1 - 2 * y)) + (x + fx * (1 - 2 * x))


def remote(src, dst, send_sem, recv_sem, device):
    return pltpu.make_async_remote_copy(src_ref=src, dst_ref=dst, send_sem=send_sem, recv_sem=recv_sem,
                                        device_id={"tp": device}, device_id_type=MESH)


def columns(device, width):
    return pl.ds(pl.multiple_of(device * width, width), width)


def gather_plan(me, xg, cw, send_sem, recv_sem):
    core, chip = lax.rem(me, 2), me // 2
    mate = me + 1 - 2 * core
    first = 2 * place(core, chip, 1 - core, core) + core
    second = 2 * place(core, chip, core, 1 - core) + core
    across = 2 * (3 - chip) + core
    rows = xg.shape[0]
    half = rows // 2

    def share(n, r0, r1, owner, device):
        block = xg.at[r0:r1, columns(owner, cw)]
        return remote(block, block, send_sem.at[n], recv_sem.at[n], device)

    near = [share(0, 0, rows, me, first), share(1, 0, rows, me, second)]
    far = [share(2, 0, half, first, second), share(3, half, rows, second, first)]
    to_mate = [share(4, 0, rows, me, mate), share(5, 0, rows, first, mate), share(6, 0, rows, second, mate),
               share(7, 0, half, across, mate), share(8, half, rows, across, mate)]
    return near, far, to_mate


def greet(me, peers):
    barrier = pltpu.get_barrier_semaphore()
    for device in peers:
        pl.semaphore_signal(barrier, inc=1, device_id={"tp": device}, device_id_type=MESH)
    pl.semaphore_wait(barrier, len(peers))


def front_kernel(layer, dims, gathered, x_hbm, bound, cos, sin, gain, wq, wk, wv, wg, wu, kc, vc, h_ref,
                 x, a, inv_ref, qkv_w, gate_w, up_w, qkv, gate, up, keys, vals, qb, ob, lb, pb, pob, x_sem, w_sem, kv_sem,
                 sums=None, sum_s=None, sum_r=None, ag_s=None, ag_r=None):
    groups, head, seq, kb, steps = dims
    qw = groups * head
    rows, width = x.shape
    ff = gate.shape[1]
    cw = kb // 2
    if gathered:
        me = lax.axis_index("tp")
        core, chip = lax.rem(me, 2), me // 2
    else:
        core, chip = 0, 0

    def sources(step):
        moved, both = (step + 2) // 3, step // 3
        swap = step // 2 * (1 - lax.rem(step, 2))
        return 2 * place(core, chip, moved, both) + swap, 2 * place(core, chip, both, moved) + 1 - swap

    def weights(step, slot):
        groups_of = ([], [], [])
        for part, device in enumerate(sources(step)):
            ks, to = columns(device, cw), slice(part * cw, (part + 1) * cw)
            pairs = (
                (0, wq.at[layer, ks, :], qkv_w.at[slot, to, 0:qw]),
                (0, wk.at[layer, ks, :], qkv_w.at[slot, to, qw:qw + head]),
                (0, wv.at[layer, ks, :], qkv_w.at[slot, to, qw + head:qw + 2 * head]),
                (1, wg.at[layer, :, ks], gate_w.at[slot, :, to]),
                (2, wu.at[layer, :, ks], up_w.at[slot, :, to]),
            )
            for n, (which, src, dst) in enumerate(pairs):
                groups_of[which].append(pltpu.make_async_copy(src, dst, w_sem.at[slot, part * 5 + n]))
        return groups_of

    def start_weights(step, slot):
        for group in weights(step, slot):
            for copy in group:
                copy.start()

    kv = [pltpu.make_async_copy(kc.at[layer], keys, kv_sem.at[0]), pltpu.make_async_copy(vc.at[layer], vals, kv_sem.at[1])]
    if gathered:
        x_copy = pltpu.make_async_copy(x_hbm, x.at[:, columns(me, cw)], x_sem)
        x_copy.start()
        start_weights(0, 0)
        near, far, to_mate = gather_plan(me, x, cw, ag_s, ag_r)
        peers = [lax.rem(me + n, 8) for n in range(1, 8)]
        greet(me, peers)
        x_copy.wait()
        for c0 in range(0, rows, 128):
            total = jnp.zeros((128, 128), F32)
            for n in range(cw // 128):
                v = x[c0:c0 + 128, pl.ds(pl.multiple_of(me * cw + n * 128, 128), 128)].astype(F32)
                total = total + v * v
            by_row = jnp.broadcast_to(jnp.sum(total, axis=-1, keepdims=True), (128, 128))
            sums[me, :, c0:c0 + 128] = by_row.T[0:8]
        swap_sums = [remote(sums.at[me], sums.at[me], sum_s.at[n], sum_r.at[n], peer) for n, peer in enumerate(peers)]
        for copy in swap_sums + near + to_mate[:1]:
            copy.start()
        for n, copy in enumerate(swap_sums):
            sender = lax.rem(me + 7 - n, 8)
            remote(sums.at[sender], sums.at[sender], sum_s.at[n], sum_r.at[n], sender).wait_recv()
        for c0 in range(0, rows, 128):
            total = sums[0, :, c0:c0 + 128]
            for n in range(1, 8):
                total = total + sums[n, :, c0:c0 + 128]
            inv = lax.rsqrt(total / width + NORM_EPS)
            inv_ref[c0:c0 + 128, :] = jnp.broadcast_to(inv[0:1], (128, 128)).T
    else:
        x_copy = pltpu.make_async_copy(x_hbm, x, x_sem)
        x_copy.start()
        start_weights(0, 0)
        x_copy.wait()

        @pl.loop(0, rows // 128)
        def _(i):
            r = pl.ds(pl.multiple_of(i * 128, 128), 128)
            total = jnp.zeros((128, 128), F32)
            for c0 in range(0, width, 128):
                v = x[r, c0:c0 + 128].astype(F32)
                total = total + v * v
            mean = jnp.sum(total, axis=-1, keepdims=True) / width
            inv_ref[r, :] = jnp.broadcast_to(lax.rsqrt(mean + NORM_EPS), (128, 128))

    @pl.loop(0, steps)
    def _(step):
        slot = lax.rem(step, 2)
        if gathered:
            for n in range(3):
                @pl.when(step == n)
                def _(n=n):
                    to_mate[n].wait_recv()

            @pl.when(step == 3)
            def _():
                to_mate[3].wait_recv()
                to_mate[4].wait_recv()

        devices = sources(step)

        @pl.loop(0, rows // 64)
        def _(i):
            r = pl.ds(pl.multiple_of(i * 64, 64), 64)
            inv = inv_ref[r, :]
            for part, device in enumerate(devices):
                for c0 in range(0, cw, 128):
                    cs = pl.ds(pl.multiple_of(device * cw + c0, 128), 128)
                    a[r, part * cw + c0:part * cw + c0 + 128] = (x[r, cs].astype(F32) * inv * gain[layer:layer + 1, cs]).astype(BF)

        first = step == 0
        w_copies = weights(step, slot)
        for copy in w_copies[0]:
            copy.wait()
        part = jnp.dot(a[...], qkv_w[slot], preferred_element_type=F32)
        qkv[...] = jnp.where(first, 0.0, qkv[...]) + part
        for copy in w_copies[1]:
            copy.wait()

        @pl.when(step + 1 < steps)
        def _():
            start_weights(step + 1, 1 - slot)

        @pl.when(step == steps - 1)
        def _():
            for copy in kv:
                copy.start()

        part = lax.dot_general(a[...], gate_w[slot], NT_DIMS, preferred_element_type=F32)
        gate[...] = jnp.where(first, 0.0, gate[...]) + part
        if gathered:
            @pl.when(step == 0)
            def _():
                near[0].wait_recv()
                to_mate[1].start()
                far[0].start()
        for copy in w_copies[2]:
            copy.wait()
        part = lax.dot_general(a[...], up_w[slot], NT_DIMS, preferred_element_type=F32)
        up[...] = jnp.where(first, 0.0, up[...]) + part
        if gathered:
            @pl.when(step == 1)
            def _():
                near[1].wait_recv()
                to_mate[2].start()
                far[1].start()

            @pl.when(step == 2)
            def _():
                far[0].wait_recv()
                to_mate[3].start()
                far[1].wait_recv()
                to_mate[4].start()

    if gathered:
        for copy in swap_sums + near + far + to_mate:
            copy.wait_send()

    @pl.loop(0, rows // 32)
    def _(i):
        r = pl.ds(pl.multiple_of(i * 32, 32), 32)
        g_in = gate[r, :].astype(BF).astype(F32)
        u_in = up[r, :].astype(BF).astype(F32)
        h_ref[r, qw:qw + ff] = (g_in * (1.0 / (1.0 + jnp.exp(-g_in))) * u_in).astype(BF)

    for copy in kv:
        copy.wait()
    attention(qkv, cos, sin, bound, keys, vals, h_ref, (qb, ob, lb, pb, pob), groups, head, seq)


def front_call(layer, dims, rows, width, qw, ff, name, gathered=False):
    groups, head, seq, kb, _ = dims
    hbm = pl.BlockSpec(memory_space=pl.ANY)
    vmem = pl.BlockSpec(memory_space=pltpu.VMEM)
    dma = pltpu.SemaphoreType.DMA
    lanes = groups * 8
    return pl.pallas_call(
        functools.partial(front_kernel, layer, dims, gathered),
        out_shape=jax.ShapeDtypeStruct((rows, qw + ff), BF),
        in_specs=[hbm, vmem, vmem, vmem, vmem] + [hbm] * 7,
        out_specs=vmem,
        scratch_shapes=[
            pltpu.VMEM((rows, width), BF), pltpu.VMEM((rows, kb), BF), pltpu.VMEM((rows, 128), F32),
            pltpu.VMEM((2, kb, qw + 2 * head), BF), pltpu.VMEM((2, ff, kb), BF), pltpu.VMEM((2, ff, kb), BF),
            pltpu.VMEM((rows, qw + 2 * head), F32), pltpu.VMEM((rows, ff), F32), pltpu.VMEM((rows, ff), F32),
            pltpu.VMEM((rows * seq, head), BF), pltpu.VMEM((rows * seq, head), BF),
            pltpu.VMEM((2, PER, lanes, head), F32), pltpu.VMEM((2, PER, lanes, 128), F32),
            pltpu.VMEM((2, PER, lanes, 8 * seq), F32), pltpu.VMEM((2, PER, lanes, 8 * seq), F32),
            pltpu.VMEM((2, PER, lanes, 128), F32),
            dma, dma((2, 10)), dma((2,)),
        ] + ([pltpu.VMEM((8, 8, rows), F32), dma((7,)), dma((7,)), dma((9,)), dma((9,))] if gathered else []),
        compiler_params=pltpu.CompilerParams(vmem_limit_bytes=63 * 2**20, **({"collective_id": 2, "has_side_effects": True} if gathered else {})),
        name=name,
    )


UNITS = ((0, 0, 256), (0, 256, 640), (1, 0, 640), (2, 0, 640), (3, 0, 640))


def back_kernel(layer, dims, last, h_hbm, x_hbm, wo, wd, out_ref, h, w, send_p, recv_p, own_p, send_i, recv_i, x_own,
                h_sem, w_sem, x_sem, pair_s, pair_r, ici_s, ici_r, xg=None, ag_s=None, ag_r=None, out_sem=None):
    cw, qw = dims
    rows, ff = h.shape[0], h.shape[1] - qw
    me = lax.axis_index("tp")
    core, chip = lax.rem(me, 2), me // 2
    mate = me + 1 - 2 * core
    order = (place(core, chip, 1, 1), place(core, chip, 0, 1), place(core, chip, 1, 0), chip)
    n_units = len(UNITS)

    def weights(u):
        i, c0, c1 = UNITS[u]
        copies = []
        for n, device in enumerate((2 * order[i] + 1 - core, 2 * order[i] + core)):
            at = 2 * c0 + n * (c1 - c0)
            for m, (src, r0, r1) in enumerate(((wo, 0, qw), (wd, qw, qw + ff))):
                copies.append(pltpu.make_async_copy(
                    src.at[layer, :, pl.ds(pl.multiple_of(device * cw + c0, 128), c1 - c0)],
                    w.at[i % 2, r0:r1, at:at + c1 - c0], w_sem.at[u, 2 * n + m]))
        return copies

    h_copy = pltpu.make_async_copy(h_hbm, h, h_sem)
    h_copy.start()
    for u in range(3):
        for copy in weights(u):
            copy.start()
    x_copy = pltpu.make_async_copy(x_hbm if x_hbm.shape[1] == cw else x_hbm.at[:, columns(me, cw)], x_own, x_sem)
    x_copy.start()
    greet(me, [mate] + [2 * q + core for q in order[:3]])

    pair, ici = [], []
    for u, (i, c0, c1) in enumerate(UNITS):
        pair.append(remote(send_p.at[i, :, c0:c1], recv_p.at[i, :, c0:c1], pair_s.at[u], pair_r.at[u], mate))
        if i < 3:
            ici.append(remote(send_i.at[i, :, c0:c1], recv_i.at[i, :, c0:c1], ici_s.at[u], ici_r.at[u], 2 * order[i] + core))

    def settle(u):
        i, c0, c1 = UNITS[u]
        pair[u].wait_recv()
        if i < 3:
            @pl.loop(0, rows // 64)
            def _(n):
                r = pl.ds(pl.multiple_of(n * 64, 64), 64)
                send_i[i, r, c0:c1] = (own_p[i, r, c0:c1] + recv_p[i, r, c0:c1]).astype(BF)
            ici[u].start()

    h_copy.wait()
    for u, (i, c0, c1) in enumerate(UNITS):
        for copy in weights(u):
            copy.wait()
        part = jnp.dot(h[...], w[i % 2, :, 2 * c0:2 * c1], preferred_element_type=F32)
        send_p[i, :, c0:c1] = part[:, 0:c1 - c0]
        pair[u].start()
        own_p[i, :, c0:c1] = part[:, c1 - c0:]
        if u == n_units - 1 or UNITS[u + 1][0] != i:
            for v in range(n_units):
                if UNITS[v][0] == i + 2:
                    for copy in weights(v):
                        copy.start()
        if u >= 1:
            settle(u - 1)
    settle(n_units - 1)
    x_copy.wait()
    for copy in ici:
        copy.wait_recv()

    @pl.loop(0, rows // 64)
    def _(n):
        r = pl.ds(pl.multiple_of(n * 64, 64), 64)
        total = own_p[3, r, :] + recv_p[3, r, :]
        for i in range(3):
            total = total + recv_i[i, r, :].astype(F32)
        new = (x_own[r, :].astype(F32) + total).astype(BF)
        if last:
            xg[r, columns(me, cw)] = new
        else:
            out_ref[r, :] = new

    if last:
        near, far, to_mate = gather_plan(me, xg, cw, ag_s, ag_r)
        for copy in near + to_mate[:1]:
            copy.start()
        for n in range(2):
            near[n].wait_recv()
            far[n].start()
            to_mate[1 + n].start()
        for n in range(2):
            far[n].wait_recv()
            to_mate[3 + n].start()
        for copy in to_mate:
            copy.wait_recv()
        out = pltpu.make_async_copy(xg, out_ref, out_sem)
        out.start()
        for copy in near + far + to_mate:
            copy.wait_send()
        out.wait()
    for copy in pair + ici:
        copy.wait_send()


def back_call(layer, name, cid, last=True, rows=512, width=5120, cw=640, qw=640, ff=1728):
    hbm = pl.BlockSpec(memory_space=pl.ANY)
    dma = pltpu.SemaphoreType.DMA
    n = len(UNITS)
    return pl.pallas_call(
        functools.partial(back_kernel, layer, (cw, qw), last),
        out_shape=jax.ShapeDtypeStruct((rows, width if last else cw), BF),
        in_specs=[hbm, hbm, hbm, hbm],
        out_specs=hbm if last else pl.BlockSpec(memory_space=pltpu.VMEM),
        scratch_shapes=[
            pltpu.VMEM((rows, qw + ff), BF), pltpu.VMEM((2, qw + ff, 2 * cw), BF),
            pltpu.VMEM((4, rows, cw), F32), pltpu.VMEM((4, rows, cw), F32), pltpu.VMEM((4, rows, cw), F32),
            pltpu.VMEM((3, rows, cw), BF), pltpu.VMEM((3, rows, cw), BF), pltpu.VMEM((rows, cw), BF),
            dma, dma((n, 4)), dma, dma((n,)), dma((n,)), dma((n,)), dma((n,)),
        ] + ([pltpu.VMEM((rows, width), BF), dma((9,)), dma((9,)), dma] if last else []),
        compiler_params=pltpu.CompilerParams(vmem_limit_bytes=60 * 2**20, collective_id=cid, has_side_effects=True),
        name=name,
    )


def solution(mesh):
    tp = mesh.shape["tp"]
    arg_specs = (P("dp", None), P("dp"), P(), P(None, None, "tp"), P(None, None, "tp"), P(None, None, "tp"), P(None, "tp", None), P(None, None, "tp"), P(None, None, "tp"), P(None, "tp", None), P(None, "dp", None, "tp", None), P(None, "dp", None, "tp", None))

    def per_device(x_in, lengths, norm_gain, w_q, w_k, w_v, w_o, w_gate, w_up, w_down, k_cache, v_cache):
        rows, width = x_in.shape
        layers, _, seq, _, head = k_cache.shape
        qw, ff = w_q.shape[-1], w_gate.shape[-1]
        groups = qw // head
        cw = width // tp
        kb = 2 * cw
        inv_freq = 1.0 / (ROPE_BASE ** (jnp.arange(0, head, 2).astype(F32) / head))
        angles = lengths.astype(F32)[:, None] * inv_freq[None, :]
        cos, sin = jnp.cos(angles), jnp.sin(angles)
        cos = jnp.concatenate([cos, cos], axis=1)
        sin = jnp.concatenate([-sin, sin], axis=1)
        bound = jnp.broadcast_to(lengths[:, None], (rows, 128))
        gain = norm_gain.astype(F32)
        gate_t, up_t = jnp.swapaxes(w_gate, 1, 2), jnp.swapaxes(w_up, 1, 2)
        kc = k_cache.reshape(layers, rows * seq, head)
        vc = v_cache.reshape(layers, rows * seq, head)
        x = x_in
        for layer in range(layers):
            last = layer == layers - 1
            dims = (groups, head, seq, kb, width // kb)
            h = front_call(layer, dims, rows, width, qw, ff, f"front{layer}", layer > 0)(
                x, bound, cos, sin, gain, w_q, w_k, w_v, gate_t, up_t, kc, vc)
            x = back_call(layer, f"back{layer}", layer, last, rows, width, cw, qw, ff)(h, x, w_o, w_down)
        return x

    return jax.shard_map(per_device, mesh=mesh, in_specs=arg_specs, out_specs=P("dp", None), check_vma=False)
```

```python
import functools

import jax
import jax.numpy as jnp
import numpy as np
from jax import lax
from jax.experimental import pallas as pl
from jax.experimental.pallas import tpu as pltpu
from jax.sharding import PartitionSpec as P

NORM_EPS = 1e-5
ROPE_BASE = 500000.0
MESH = pl.DeviceIdType.MESH
BF, F32 = jnp.bfloat16, jnp.float32
PER = 4
NT_DIMS = (((1,), (1,)), ((), ()))


def angle_table(seq, head):
    freq = np.float32(1.0) / np.power(np.float32(ROPE_BASE), np.arange(0, head, 2, dtype=np.float32) / np.float32(head))
    angle = np.arange(seq, dtype=np.float32)[:, None] * freq[None, :]
    cos, sin = np.cos(angle.astype(np.float64)), np.sin(angle.astype(np.float64))
    table = np.zeros((128, 2 * head), np.float32)
    table[:seq] = np.concatenate([cos, cos, -sin, sin], axis=1)
    return table


def rotate(qkv, lens, table, groups, head):
    at = lax.broadcasted_iota(jnp.int32, (head, head), 0)
    to = lax.broadcasted_iota(jnp.int32, (head, head), 1)
    swap = (at == lax.rem(to + head // 2, head)).astype(BF)

    @pl.loop(0, qkv.shape[0] // 128)
    def _(i):
        r = pl.ds(pl.multiple_of(i * 128, 128), 128)
        spot = lax.broadcasted_iota(jnp.int32, (128, 128), 1).astype(F32)
        hot = (lens[r, :] == spot).astype(F32)
        angle = jnp.dot(hot, table[...], precision=lax.Precision.HIGHEST, preferred_element_type=F32)
        c, s = angle[:, 0:head], angle[:, head:2 * head]
        for j in range(groups + 1):
            v = qkv[r, head * j:head * (j + 1)].astype(BF)
            other = jnp.dot(v, swap, preferred_element_type=F32)
            qkv[r, head * j:head * (j + 1)] = v.astype(F32) * c + other * s


def attention(qkv, lens, keys, vals, h_ref, bufs, groups, head, seq):
    lb, pb = bufs
    per = lb.shape[1]
    span = 8 * seq
    n_groups = qkv.shape[0] // (8 * per)
    scale = head ** -0.5
    col = lax.broadcasted_iota(jnp.int32, (8, span), 1).astype(F32)
    low = (lax.broadcasted_iota(jnp.int32, (8, span), 0) * seq).astype(F32)
    own = lax.broadcasted_iota(jnp.int32, (8, 128), 0) == lax.broadcasted_iota(jnp.int32, (8, 128), 1)
    none = jnp.zeros((120, head), BF)

    def block(g, n):
        t0 = pl.multiple_of(g * (8 * per) + 8 * n, 8)
        return t0, pl.ds(t0, 8), pl.ds(pl.multiple_of(t0 * seq, span), span)

    def score(g):
        slot = lax.rem(g, 2)
        for n in range(per):
            t0, rows, cached = block(g, n)
            q = jnp.concatenate([qkv[rows, head * j:head * (j + 1)] for j in range(groups)], axis=0).astype(BF)
            k_new = jnp.concatenate([qkv[rows, groups * head:(groups + 1) * head].astype(BF), none], axis=0)
            old = lax.dot_general(q, keys[cached, :], NT_DIMS, preferred_element_type=F32) * scale
            new = lax.dot_general(q, k_new, NT_DIMS, preferred_element_type=F32) * scale
            high = jnp.concatenate([lens[rows, :]] * (span // 128), axis=1) + low
            keep = (col >= low) & (col < high)
            for j in range(groups):
                r = slice(8 * j, 8 * (j + 1))
                lb[slot, n, r, 0:span] = jnp.where(keep, old[r], -jnp.inf)
                lb[slot, n, r, span:] = jnp.where(own, new[r], -jnp.inf)

    def weigh(g):
        slot = lax.rem(g, 2)
        for n in range(per):
            for j in range(groups):
                r = slice(8 * j, 8 * (j + 1))
                logits = [lb[slot, n, r, c0:c0 + 128] for c0 in range(0, span + 128, 128)]
                peak = jnp.max(functools.reduce(jnp.maximum, logits), axis=-1, keepdims=True)
                w = [jnp.exp(v - peak) for v in logits]
                inv = 1.0 / jnp.sum(functools.reduce(jnp.add, w), axis=-1, keepdims=True)
                for m, v in enumerate(w):
                    pb[slot, n, r, 128 * m:128 * (m + 1)] = v * inv

    def mix(g):
        slot = lax.rem(g, 2)
        for n0 in range(0, per, 2):
            outs = []
            for n in (n0, n0 + 1):
                t0, rows, cached = block(g, n)
                p = pb[slot, n].astype(BF)
                v_new = jnp.concatenate([qkv[rows, (groups + 1) * head:].astype(BF), none], axis=0)
                outs.append(jnp.dot(p[:, 0:span], vals[cached, :], preferred_element_type=F32)
                            + jnp.dot(p[:, span:], v_new, preferred_element_type=F32))
            rows = pl.ds(pl.multiple_of(block(g, n0)[0], 16), 16)
            for j in range(groups):
                both = jnp.concatenate([o[8 * j:8 * (j + 1)] for o in outs], axis=0).astype(BF)
                h_ref[rows, head * j:head * (j + 1)] = both

    @pl.loop(0, n_groups + 2)
    def _(i):
        for lag, stage in ((2, mix), (1, weigh), (0, score)):
            stage(jnp.clip(i - lag, 0, n_groups - 1))


def place(core, chip, fx, fy):
    x, y = lax.rem(chip, 2), chip // 2
    return 2 * (y + fy * (1 - 2 * y)) + (x + fx * (1 - 2 * x))


def remote(src, dst, send_sem, recv_sem, device):
    return pltpu.make_async_remote_copy(src_ref=src, dst_ref=dst, send_sem=send_sem, recv_sem=recv_sem,
                                        device_id={"tp": device}, device_id_type=MESH)


def columns(device, width):
    return pl.ds(pl.multiple_of(device * width, width), width)


def gather_plan(me, xg, cw, send_sem, recv_sem):
    core, chip = lax.rem(me, 2), me // 2
    mate = me + 1 - 2 * core
    first = 2 * place(core, chip, 1 - core, core) + core
    second = 2 * place(core, chip, core, 1 - core) + core
    across = 2 * (3 - chip) + core
    rows = xg.shape[0]
    half = rows // 2

    def share(n, r0, r1, owner, device):
        block = xg.at[r0:r1, columns(owner, cw)]
        return remote(block, block, send_sem.at[n], recv_sem.at[n], device)

    near = [share(0, 0, rows, me, first), share(1, 0, rows, me, second)]
    far = [share(2, 0, half, first, second), share(3, half, rows, second, first)]
    to_mate = [share(4, 0, rows, me, mate), share(5, 0, rows, first, mate), share(6, 0, rows, second, mate),
               share(7, 0, half, across, mate), share(8, half, rows, across, mate)]
    return near, far, to_mate


def greet(me, peers):
    barrier = pltpu.get_barrier_semaphore()
    for device in peers:
        pl.semaphore_signal(barrier, inc=1, device_id={"tp": device}, device_id_type=MESH)
    pl.semaphore_wait(barrier, len(peers))


def front_kernel(layer, dims, gathered, x_hbm, lens, table, gain, wq, wk, wv, wg, wu, kc, vc, h_ref,
                 x, a, inv_ref, qkv_w, gate_w, up_w, qkv, gate, up, keys, vals, lb, pb, x_sem, w_sem, kv_sem,
                 sums=None, sum_s=None, sum_r=None, ag_s=None, ag_r=None):
    groups, head, seq, kb, steps = dims
    qw = groups * head
    rows, width = x.shape
    ff = gate.shape[1]
    cw = kb // 2
    if gathered:
        me = lax.axis_index("tp")
        core, chip = lax.rem(me, 2), me // 2
    else:
        core, chip = 0, 0

    def sources(step):
        moved, both = (step + 2) // 3, step // 3
        swap = step // 2 * (1 - lax.rem(step, 2))
        return 2 * place(core, chip, moved, both) + swap, 2 * place(core, chip, both, moved) + 1 - swap

    def weights(step, slot):
        groups_of = ([], [], [])
        for part, device in enumerate(sources(step)):
            ks, to = columns(device, cw), slice(part * cw, (part + 1) * cw)
            pairs = (
                (0, wq.at[layer, ks, :], qkv_w.at[slot, to, 0:qw]),
                (0, wk.at[layer, ks, :], qkv_w.at[slot, to, qw:qw + head]),
                (0, wv.at[layer, ks, :], qkv_w.at[slot, to, qw + head:qw + 2 * head]),
                (1, wg.at[layer, :, ks], gate_w.at[slot, :, to]),
                (2, wu.at[layer, :, ks], up_w.at[slot, :, to]),
            )
            for n, (which, src, dst) in enumerate(pairs):
                groups_of[which].append(pltpu.make_async_copy(src, dst, w_sem.at[slot, part * 5 + n]))
        return groups_of

    def start_weights(step, slot):
        for group in weights(step, slot):
            for copy in group:
                copy.start()

    kv = [pltpu.make_async_copy(kc.at[layer], keys, kv_sem.at[0]), pltpu.make_async_copy(vc.at[layer], vals, kv_sem.at[1])]
    if gathered:
        x_copy = pltpu.make_async_copy(x_hbm, x.at[:, columns(me, cw)], x_sem)
        x_copy.start()
        start_weights(0, 0)
        near, far, to_mate = gather_plan(me, x, cw, ag_s, ag_r)
        peers = [lax.rem(me + n, 8) for n in range(1, 8)]
        greet(me, peers)
        x_copy.wait()
        for c0 in range(0, rows, 128):
            total = jnp.zeros((128, 128), F32)
            for n in range(cw // 128):
                v = x[c0:c0 + 128, pl.ds(pl.multiple_of(me * cw + n * 128, 128), 128)].astype(F32)
                total = total + v * v
            by_row = jnp.broadcast_to(jnp.sum(total, axis=-1, keepdims=True), (128, 128))
            sums[me, :, c0:c0 + 128] = by_row.T[0:8]
        swap_sums = [remote(sums.at[me], sums.at[me], sum_s.at[n], sum_r.at[n], peer) for n, peer in enumerate(peers)]
        for copy in swap_sums + near[:1] + to_mate[:1]:
            copy.start()
        for n, copy in enumerate(swap_sums):
            sender = lax.rem(me + 7 - n, 8)
            remote(sums.at[sender], sums.at[sender], sum_s.at[n], sum_r.at[n], sender).wait_recv()
        for c0 in range(0, rows, 128):
            total = sums[0, :, c0:c0 + 128]
            for n in range(1, 8):
                total = total + sums[n, :, c0:c0 + 128]
            inv = lax.rsqrt(total / width + NORM_EPS)
            inv_ref[c0:c0 + 128, :] = jnp.broadcast_to(inv[0:1], (128, 128)).T
    else:
        x_copy = pltpu.make_async_copy(x_hbm, x, x_sem)
        x_copy.start()
        early = weights(0, 0)
        for copy in early[0]:
            copy.start()
        x_copy.wait()
        for copy in early[1] + early[2]:
            copy.start()

        @pl.loop(0, rows // 128)
        def _(i):
            r = pl.ds(pl.multiple_of(i * 128, 128), 128)
            total = jnp.zeros((128, 128), F32)
            for c0 in range(0, width, 128):
                v = x[r, c0:c0 + 128].astype(F32)
                total = total + v * v
            mean = jnp.sum(total, axis=-1, keepdims=True) / width
            inv_ref[r, :] = jnp.broadcast_to(lax.rsqrt(mean + NORM_EPS), (128, 128))

    @pl.loop(0, steps)
    def _(step):
        slot = lax.rem(step, 2)
        if gathered:
            for n in range(3):
                @pl.when(step == n)
                def _(n=n):
                    to_mate[n].wait_recv()

            @pl.when(step == 3)
            def _():
                to_mate[3].wait_recv()
                to_mate[4].wait_recv()

        devices = sources(step)

        @pl.loop(0, rows // 64)
        def _(i):
            r = pl.ds(pl.multiple_of(i * 64, 64), 64)
            inv = inv_ref[r, :]
            for part, device in enumerate(devices):
                for c0 in range(0, cw, 128):
                    cs = pl.ds(pl.multiple_of(device * cw + c0, 128), 128)
                    a[r, part * cw + c0:part * cw + c0 + 128] = (x[r, cs].astype(F32) * inv * gain[layer:layer + 1, cs].astype(F32)).astype(BF)

        first = step == 0
        w_copies = weights(step, slot)
        for copy in w_copies[0]:
            copy.wait()
        part = jnp.dot(a[...], qkv_w[slot], preferred_element_type=F32)
        qkv[...] = jnp.where(first, 0.0, qkv[...]) + part
        for copy in w_copies[1]:
            copy.wait()

        @pl.when(step + 1 < steps)
        def _():
            start_weights(step + 1, 1 - slot)

        @pl.when(step == steps - 1)
        def _():
            for copy in kv:
                copy.start()

        part = lax.dot_general(a[...], gate_w[slot], NT_DIMS, preferred_element_type=F32)
        gate[...] = jnp.where(first, 0.0, gate[...]) + part
        if gathered:
            @pl.when(step == 0)
            def _():
                near[0].wait_send()
                near[1].start()
                near[0].wait_recv()
                to_mate[1].start()
                far[0].start()
        for copy in w_copies[2]:
            copy.wait()
        part = lax.dot_general(a[...], up_w[slot], NT_DIMS, preferred_element_type=F32)
        up[...] = jnp.where(first, 0.0, up[...]) + part
        if gathered:
            @pl.when(step == 1)
            def _():
                near[1].wait_recv()
                to_mate[2].start()
                far[1].start()

            @pl.when(step == 2)
            def _():
                far[0].wait_recv()
                to_mate[3].start()
                far[1].wait_recv()
                to_mate[4].start()

    if gathered:
        for copy in swap_sums + near[1:] + far + to_mate:
            copy.wait_send()

    @pl.loop(0, rows // 32)
    def _(i):
        r = pl.ds(pl.multiple_of(i * 32, 32), 32)
        g_in = gate[r, :].astype(BF).astype(F32)
        u_in = up[r, :].astype(BF).astype(F32)
        h_ref[r, qw:qw + ff] = (g_in * (1.0 / (1.0 + jnp.exp(-g_in))) * u_in).astype(BF)

    rotate(qkv, lens, table, groups, head)
    for copy in kv:
        copy.wait()
    attention(qkv, lens, keys, vals, h_ref, (lb, pb), groups, head, seq)


def front_call(layer, dims, rows, width, qw, ff, name, gathered=False):
    groups, head, seq, kb, _ = dims
    hbm = pl.BlockSpec(memory_space=pl.ANY)
    vmem = pl.BlockSpec(memory_space=pltpu.VMEM)
    dma = pltpu.SemaphoreType.DMA
    lanes = groups * 8
    return pl.pallas_call(
        functools.partial(front_kernel, layer, dims, gathered),
        out_shape=jax.ShapeDtypeStruct((rows, qw + ff), BF),
        in_specs=[hbm, vmem, vmem, vmem] + [hbm] * 7,
        out_specs=vmem,
        scratch_shapes=[
            pltpu.VMEM((rows, width), BF), pltpu.VMEM((rows, kb), BF), pltpu.VMEM((rows, 128), F32),
            pltpu.VMEM((2, kb, qw + 2 * head), BF), pltpu.VMEM((2, ff, kb), BF), pltpu.VMEM((2, ff, kb), BF),
            pltpu.VMEM((rows, qw + 2 * head), F32), pltpu.VMEM((rows, ff), F32), pltpu.VMEM((rows, ff), F32),
            pltpu.VMEM((rows * seq, head), BF), pltpu.VMEM((rows * seq, head), BF),
            pltpu.VMEM((2, PER, lanes, 8 * seq + 128), F32), pltpu.VMEM((2, PER, lanes, 8 * seq + 128), F32),
            dma, dma((2, 10)), dma((2,)),
        ] + ([pltpu.VMEM((8, 8, rows), F32), dma((7,)), dma((7,)), dma((9,)), dma((9,))] if gathered else []),
        compiler_params=pltpu.CompilerParams(vmem_limit_bytes=63 * 2**20, **({"collective_id": 2, "has_side_effects": True} if gathered else {})),
        name=name,
    )


UNITS = ((0, 0, 256), (0, 256, 640), (1, 0, 640), (2, 0, 640), (3, 0, 640))


def back_kernel(layer, dims, last, h_hbm, x_hbm, wo, wd, out_ref, h, w, send_p, recv_p, own_p, send_i, recv_i, x_own,
                h_sem, w_sem, x_sem, pair_s, pair_r, ici_s, ici_r, xg=None, ag_s=None, ag_r=None, out_sem=None):
    cw, qw = dims
    rows, ff = h.shape[0], h.shape[1] - qw
    me = lax.axis_index("tp")
    core, chip = lax.rem(me, 2), me // 2
    mate = me + 1 - 2 * core
    order = (place(core, chip, 1, 1), place(core, chip, 0, 1), place(core, chip, 1, 0), chip)
    n_units = len(UNITS)

    def weights(u):
        i, c0, c1 = UNITS[u]
        copies = []
        for n, device in enumerate((2 * order[i] + 1 - core, 2 * order[i] + core)):
            at = 2 * c0 + n * (c1 - c0)
            for m, (src, r0, r1) in enumerate(((wo, 0, qw), (wd, qw, qw + ff))):
                copies.append(pltpu.make_async_copy(
                    src.at[layer, :, pl.ds(pl.multiple_of(device * cw + c0, 128), c1 - c0)],
                    w.at[i % 2, r0:r1, at:at + c1 - c0], w_sem.at[u, 2 * n + m]))
        return copies

    h_copy = pltpu.make_async_copy(h_hbm, h, h_sem)
    h_copy.start()
    for u in range(3):
        for copy in weights(u):
            copy.start()
    x_copy = pltpu.make_async_copy(x_hbm if x_hbm.shape[1] == cw else x_hbm.at[:, columns(me, cw)], x_own, x_sem)
    x_copy.start()
    greet(me, [mate] + [2 * q + core for q in order[:3]])

    pair, ici = [], []
    for u, (i, c0, c1) in enumerate(UNITS):
        pair.append(remote(send_p.at[i, :, c0:c1], recv_p.at[i, :, c0:c1], pair_s.at[u], pair_r.at[u], mate))
        if i < 3:
            ici.append(remote(send_i.at[i, :, c0:c1], recv_i.at[i, :, c0:c1], ici_s.at[u], ici_r.at[u], 2 * order[i] + core))

    def settle(u):
        i, c0, c1 = UNITS[u]
        pair[u].wait_recv()
        if i < 3:
            @pl.loop(0, rows // 64)
            def _(n):
                r = pl.ds(pl.multiple_of(n * 64, 64), 64)
                send_i[i, r, c0:c1] = (own_p[i, r, c0:c1] + recv_p[i, r, c0:c1]).astype(BF)
            ici[u].start()

    h_copy.wait()
    for u, (i, c0, c1) in enumerate(UNITS):
        for copy in weights(u):
            copy.wait()
        part = jnp.dot(h[...], w[i % 2, :, 2 * c0:2 * c1], preferred_element_type=F32)
        send_p[i, :, c0:c1] = part[:, 0:c1 - c0]
        pair[u].start()
        own_p[i, :, c0:c1] = part[:, c1 - c0:]
        if u == n_units - 1 or UNITS[u + 1][0] != i:
            for v in range(n_units):
                if UNITS[v][0] == i + 2:
                    for copy in weights(v):
                        copy.start()
        if u >= 1:
            settle(u - 1)
    settle(n_units - 1)
    x_copy.wait()
    for copy in ici:
        copy.wait_recv()

    @pl.loop(0, rows // 64)
    def _(n):
        r = pl.ds(pl.multiple_of(n * 64, 64), 64)
        total = own_p[3, r, :] + recv_p[3, r, :]
        for i in range(3):
            total = total + recv_i[i, r, :].astype(F32)
        new = (x_own[r, :].astype(F32) + total).astype(BF)
        if last:
            xg[r, columns(me, cw)] = new
        else:
            out_ref[r, :] = new

    if last:
        near, far, to_mate = gather_plan(me, xg, cw, ag_s, ag_r)
        for copy in near[:1] + to_mate[:1]:
            copy.start()
        near[0].wait_send()
        near[1].start()
        for n in range(2):
            near[n].wait_recv()
            far[n].start()
            to_mate[1 + n].start()
        for n in range(2):
            far[n].wait_recv()
            to_mate[3 + n].start()
        for copy in to_mate:
            copy.wait_recv()
        out = pltpu.make_async_copy(xg, out_ref, out_sem)
        out.start()
        for copy in near[1:] + far + to_mate:
            copy.wait_send()
        out.wait()
    for copy in pair + ici:
        copy.wait_send()


def back_call(layer, name, cid, last=True, rows=512, width=5120, cw=640, qw=640, ff=1728):
    hbm = pl.BlockSpec(memory_space=pl.ANY)
    dma = pltpu.SemaphoreType.DMA
    n = len(UNITS)
    return pl.pallas_call(
        functools.partial(back_kernel, layer, (cw, qw), last),
        out_shape=jax.ShapeDtypeStruct((rows, width if last else cw), BF),
        in_specs=[hbm, hbm, hbm, hbm],
        out_specs=hbm if last else pl.BlockSpec(memory_space=pltpu.VMEM),
        scratch_shapes=[
            pltpu.VMEM((rows, qw + ff), BF), pltpu.VMEM((2, qw + ff, 2 * cw), BF),
            pltpu.VMEM((4, rows, cw), F32), pltpu.VMEM((4, rows, cw), F32), pltpu.VMEM((4, rows, cw), F32),
            pltpu.VMEM((3, rows, cw), BF), pltpu.VMEM((3, rows, cw), BF), pltpu.VMEM((rows, cw), BF),
            dma, dma((n, 4)), dma, dma((n,)), dma((n,)), dma((n,)), dma((n,)),
        ] + ([pltpu.VMEM((rows, width), BF), dma((9,)), dma((9,)), dma] if last else []),
        compiler_params=pltpu.CompilerParams(vmem_limit_bytes=60 * 2**20, collective_id=cid, has_side_effects=True),
        name=name,
    )


def solution(mesh):
    tp = mesh.shape["tp"]
    arg_specs = (P("dp", None), P("dp"), P(), P(None, None, "tp"), P(None, None, "tp"), P(None, None, "tp"), P(None, "tp", None), P(None, None, "tp"), P(None, None, "tp"), P(None, "tp", None), P(None, "dp", None, "tp", None), P(None, "dp", None, "tp", None))

    def per_device(x_in, lengths, norm_gain, w_q, w_k, w_v, w_o, w_gate, w_up, w_down, k_cache, v_cache):
        rows, width = x_in.shape
        layers, _, seq, _, head = k_cache.shape
        qw, ff = w_q.shape[-1], w_gate.shape[-1]
        groups = qw // head
        cw = width // tp
        kb = 2 * cw
        lens = jnp.broadcast_to(lengths.astype(F32)[:, None], (rows, 128))
        table = jnp.asarray(angle_table(seq, head))
        gate_t, up_t = jnp.swapaxes(w_gate, 1, 2), jnp.swapaxes(w_up, 1, 2)
        kc = k_cache.reshape(layers, rows * seq, head)
        vc = v_cache.reshape(layers, rows * seq, head)
        x = x_in
        for layer in range(layers):
            last = layer == layers - 1
            dims = (groups, head, seq, kb, width // kb)
            h = front_call(layer, dims, rows, width, qw, ff, f"front{layer}", layer > 0)(
                x, lens, table, norm_gain, w_q, w_k, w_v, gate_t, up_t, kc, vc)
            x = back_call(layer, f"back{layer}", layer, last, rows, width, cw, qw, ff)(h, x, w_o, w_down)
        return x

    return jax.shard_map(per_device, mesh=mesh, in_specs=arg_specs, out_specs=P("dp", None), check_vma=False)
```

```python
import functools
import types

import jax
import jax.numpy as jnp
import numpy as np
from jax import lax
from jax.experimental import pallas as pl
from jax.experimental.pallas import tpu as pltpu
from jax.sharding import PartitionSpec as P

NORM_EPS = 1e-5
ROPE_BASE = 500000.0
MESH = pl.DeviceIdType.MESH
BF, F32 = jnp.bfloat16, jnp.float32
PER = 4
NT_DIMS = (((1,), (1,)), ((), ()))


def angle_table(seq, head):
    freq = np.float32(1.0) / np.power(np.float32(ROPE_BASE), np.arange(0, head, 2, dtype=np.float32) / np.float32(head))
    angle = np.arange(seq, dtype=np.float32)[:, None] * freq[None, :]
    cos, sin = np.cos(angle.astype(np.float64)), np.sin(angle.astype(np.float64))
    table = np.zeros((128, 2 * head), np.float32)
    table[:seq] = np.concatenate([cos, cos, -sin, sin], axis=1)
    return table


def rotate(qkv, lens, table, groups, head):
    at = lax.broadcasted_iota(jnp.int32, (head, head), 0)
    to = lax.broadcasted_iota(jnp.int32, (head, head), 1)
    swap = (at == lax.rem(to + head // 2, head)).astype(BF)

    @pl.loop(0, qkv.shape[0] // 128)
    def _(i):
        r = pl.ds(pl.multiple_of(i * 128, 128), 128)
        spot = lax.broadcasted_iota(jnp.int32, (128, 128), 1).astype(F32)
        hot = (lens[r, :] == spot).astype(F32)
        angle = jnp.dot(hot, table[...], precision=lax.Precision.HIGHEST, preferred_element_type=F32)
        c, s = angle[:, 0:head], angle[:, head:2 * head]
        for j in range(groups + 1):
            v = qkv[r, head * j:head * (j + 1)].astype(BF)
            other = jnp.dot(v, swap, preferred_element_type=F32)
            qkv[r, head * j:head * (j + 1)] = v.astype(F32) * c + other * s


def attention(qkv, lens, keys, vals, h_ref, bufs, groups, head, seq):
    lb, pb = bufs
    per = lb.shape[1]
    span = 8 * seq
    n_groups = qkv.shape[0] // (8 * per)
    scale = head ** -0.5
    col = lax.broadcasted_iota(jnp.int32, (8, span), 1).astype(F32)
    low = (lax.broadcasted_iota(jnp.int32, (8, span), 0) * seq).astype(F32)
    own = lax.broadcasted_iota(jnp.int32, (8, 128), 0) == lax.broadcasted_iota(jnp.int32, (8, 128), 1)
    none = jnp.zeros((120, head), BF)

    def block(g, n):
        t0 = pl.multiple_of(g * (8 * per) + 8 * n, 8)
        return t0, pl.ds(t0, 8), pl.ds(pl.multiple_of(t0 * seq, span), span)

    def score(g):
        slot = lax.rem(g, 2)
        for n in range(per):
            t0, rows, cached = block(g, n)
            q = jnp.concatenate([qkv[rows, head * j:head * (j + 1)] for j in range(groups)], axis=0).astype(BF)
            k_new = jnp.concatenate([qkv[rows, groups * head:(groups + 1) * head].astype(BF), none], axis=0)
            old = lax.dot_general(q, keys[cached, :], NT_DIMS, preferred_element_type=F32) * scale
            new = lax.dot_general(q, k_new, NT_DIMS, preferred_element_type=F32) * scale
            high = jnp.concatenate([lens[rows, :]] * (span // 128), axis=1) + low
            keep = (col >= low) & (col < high)
            for j in range(groups):
                r = slice(8 * j, 8 * (j + 1))
                lb[slot, n, r, 0:span] = jnp.where(keep, old[r], -jnp.inf)
                lb[slot, n, r, span:] = jnp.where(own, new[r], -jnp.inf)

    def weigh(g):
        slot = lax.rem(g, 2)
        for n in range(per):
            for j in range(groups):
                r = slice(8 * j, 8 * (j + 1))
                logits = [lb[slot, n, r, c0:c0 + 128] for c0 in range(0, span + 128, 128)]
                peak = jnp.max(functools.reduce(jnp.maximum, logits), axis=-1, keepdims=True)
                w = [jnp.exp(v - peak) for v in logits]
                inv = 1.0 / jnp.sum(functools.reduce(jnp.add, w), axis=-1, keepdims=True)
                for m, v in enumerate(w):
                    pb[slot, n, r, 128 * m:128 * (m + 1)] = v * inv

    def mix(g):
        slot = lax.rem(g, 2)
        for n0 in range(0, per, 2):
            outs = []
            for n in (n0, n0 + 1):
                t0, rows, cached = block(g, n)
                p = pb[slot, n].astype(BF)
                v_new = jnp.concatenate([qkv[rows, (groups + 1) * head:].astype(BF), none], axis=0)
                outs.append(jnp.dot(p[:, 0:span], vals[cached, :], preferred_element_type=F32)
                            + jnp.dot(p[:, span:], v_new, preferred_element_type=F32))
            rows = pl.ds(pl.multiple_of(block(g, n0)[0], 16), 16)
            for j in range(groups):
                both = jnp.concatenate([o[8 * j:8 * (j + 1)] for o in outs], axis=0).astype(BF)
                h_ref[rows, head * j:head * (j + 1)] = both

    @pl.loop(0, n_groups + 2)
    def _(i):
        for lag, stage in ((2, mix), (1, weigh), (0, score)):
            stage(jnp.clip(i - lag, 0, n_groups - 1))


def place(core, chip, fx, fy):
    x, y = lax.rem(chip, 2), chip // 2
    return 2 * (y + fy * (1 - 2 * y)) + (x + fx * (1 - 2 * x))


def remote(src, dst, send_sem, recv_sem, device):
    return pltpu.make_async_remote_copy(src_ref=src, dst_ref=dst, send_sem=send_sem, recv_sem=recv_sem,
                                        device_id={"tp": device}, device_id_type=MESH)


def columns(device, width):
    return pl.ds(pl.multiple_of(device * width, width), width)


def gather_plan(me, xg, cw, send_sem, recv_sem):
    core, chip = lax.rem(me, 2), me // 2
    mate = me + 1 - 2 * core
    first = 2 * place(core, chip, 1 - core, core) + core
    second = 2 * place(core, chip, core, 1 - core) + core
    across = 2 * (3 - chip) + core
    rows = xg.shape[0]
    half = rows // 2

    def share(n, r0, r1, owner, device):
        block = xg.at[r0:r1, columns(owner, cw)]
        return remote(block, block, send_sem.at[n], recv_sem.at[n], device)

    near = [share(0, 0, rows, me, first), share(1, 0, rows, me, second)]
    far = [share(2, 0, half, first, second), share(3, half, rows, second, first)]
    to_mate = [share(4, 0, rows, me, mate), share(5, 0, rows, first, mate), share(6, 0, rows, second, mate),
               share(7, 0, half, across, mate), share(8, half, rows, across, mate)]
    return near, far, to_mate


def greet(me, peers):
    barrier = pltpu.get_barrier_semaphore()
    for device in peers:
        pl.semaphore_signal(barrier, inc=1, device_id={"tp": device}, device_id_type=MESH)
    pl.semaphore_wait(barrier, len(peers))


UNITS = ((0, 0, 256), (0, 256, 640), (1, 0, 640), (2, 0, 640), (3, 0, 640))
SCRATCH = ("x", "a", "inv", "qkv_w", "gate_w", "up_w", "wo_w", "qkv", "gate", "up", "keys", "vals", "lb", "pb", "h", "recv_p",
           "recv_i", "sums", "x_sem", "w_sem", "kv_sem", "out_w_sem", "pair_s", "pair_r", "ici_s", "ici_r", "sum_s", "sum_r",
           "ag_s", "ag_r", "out_sem")


def block_kernel(dims, x_hbm, lens, table, gain, wq, wk, wv, wg, wu, wo, wd, kc, vc, out_ref, *scratch):
    layers, groups, head, seq, cw, steps = dims
    m = types.SimpleNamespace(**dict(zip(SCRATCH, scratch, strict=True)))
    x, h = m.x, m.h
    rows, width = x.shape
    qw, ff, kb = groups * head, m.gate.shape[1], 2 * cw
    n_units, n_peers = len(UNITS), width // cw
    me = lax.axis_index("tp")
    core, chip = lax.rem(me, 2), me // 2
    mate = me + 1 - 2 * core
    order = (place(core, chip, 1, 1), place(core, chip, 0, 1), place(core, chip, 1, 0), chip)
    peers = [lax.rem(me + n, n_peers) for n in range(1, n_peers)]
    chunks = cw // 128

    def start(copies):
        for copy in copies:
            copy.start()

    def sources(step):
        moved, both = (step + 2) // 3, step // 3
        swap = step // 2 * (1 - lax.rem(step, 2))
        return 2 * place(core, chip, moved, both) + swap, 2 * place(core, chip, both, moved) + 1 - swap

    def in_weights(layer, step, slot):
        found = ([], [], [])
        for part, device in enumerate(sources(step)):
            ks, to = columns(device, cw), slice(part * cw, (part + 1) * cw)
            pairs = (
                (0, wq.at[layer, ks, :], m.qkv_w.at[slot, to, 0:qw]),
                (0, wk.at[layer, ks, :], m.qkv_w.at[slot, to, qw:qw + head]),
                (0, wv.at[layer, ks, :], m.qkv_w.at[slot, to, qw + head:qw + 2 * head]),
                (1, wg.at[layer, :, ks], m.gate_w.at[slot, :, to]),
                (2, wu.at[layer, :, ks], m.up_w.at[slot, :, to]),
            )
            for n, (which, src, dst) in enumerate(pairs):
                found[which].append(pltpu.make_async_copy(src, dst, m.w_sem.at[slot, part * 5 + n]))
        return found

    def down_w(i):
        return (m.gate_w, m.up_w)[i % 2].at[i // 2]

    def out_weights(layer, u, which):
        i, c0, c1 = UNITS[u]
        copies = []
        for n, device in enumerate((2 * order[i] + 1 - core, 2 * order[i] + core)):
            at = 2 * c0 + n * (c1 - c0)
            src, dst = ((wd, down_w(i)), (wo, m.wo_w.at[i % 2]))[which]
            copies.append(pltpu.make_async_copy(
                src.at[layer, :, pl.ds(pl.multiple_of(device * cw + c0, 128), c1 - c0)],
                dst.at[:, at:at + c1 - c0], m.out_w_sem.at[u, 2 * which + n]))
        return copies

    def start_out_weights(layer, tiles, whiches):
        for u, (i, _, _) in enumerate(UNITS):
            if i in tiles:
                for which in whiches:
                    start(out_weights(layer, u, which))

    def front(layer, gather):
        kv = [pltpu.make_async_copy(kc.at[layer], m.keys, m.kv_sem.at[0]),
              pltpu.make_async_copy(vc.at[layer], m.vals, m.kv_sem.at[1])]
        if gather:
            near, far, to_mate = gather

        @pl.loop(0, steps)
        def _(step):
            slot = lax.rem(step, 2)
            if gather:
                for n in range(3):
                    @pl.when(step == n)
                    def _(n=n):
                        to_mate[n].wait_recv()

                @pl.when(step == 3)
                def _():
                    to_mate[3].wait_recv()
                    to_mate[4].wait_recv()

            devices = sources(step)

            @pl.loop(0, rows // 64)
            def _(i):
                r = pl.ds(pl.multiple_of(i * 64, 64), 64)
                inv = m.inv[r, :]
                for part, device in enumerate(devices):
                    for c0 in range(0, cw, 128):
                        cs = pl.ds(pl.multiple_of(device * cw + c0, 128), 128)
                        g = gain[layer:layer + 1, cs].astype(F32)
                        m.a[r, part * cw + c0:part * cw + c0 + 128] = (x[r, cs].astype(F32) * inv * g).astype(BF)

            first = step == 0
            w_copies = in_weights(layer, step, slot)
            for copy in w_copies[0]:
                copy.wait()
            part = jnp.dot(m.a[...], m.qkv_w[slot], preferred_element_type=F32)
            m.qkv[...] = jnp.where(first, 0.0, m.qkv[...]) + part
            for copy in w_copies[1]:
                copy.wait()
            if not gather:
                @pl.when(first)
                def _():
                    for copies in in_weights(layer, 1, 1):
                        start(copies)

            part = lax.dot_general(m.a[...], m.gate_w[slot], NT_DIMS, preferred_element_type=F32)
            m.gate[...] = jnp.where(first, 0.0, m.gate[...]) + part
            if gather:
                @pl.when(step == 0)
                def _():
                    near[0].wait_send()
                    near[1].start()
                    near[0].wait_recv()
                    to_mate[1].start()
                    far[0].start()
            for copy in w_copies[2]:
                copy.wait()
            part = lax.dot_general(m.a[...], m.up_w[slot], NT_DIMS, preferred_element_type=F32)
            m.up[...] = jnp.where(first, 0.0, m.up[...]) + part
            if gather:
                @pl.when(step == 1)
                def _():
                    near[1].wait_recv()
                    to_mate[2].start()
                    far[1].start()

                @pl.when(step == 2)
                def _():
                    far[0].wait_recv()
                    to_mate[3].start()
                    far[1].wait_recv()
                    to_mate[4].start()

            @pl.when(step + 2 < steps)
            def _():
                for copies in in_weights(layer, step + 2, slot):
                    start(copies)

            @pl.when(step == 1)
            def _():
                start(kv)

            @pl.when(step == 2)
            def _():
                start_out_weights(layer, (0, 1), (0, 1))

        if gather:
            for copy in near[1:] + far + to_mate:
                copy.wait_send()
        start_out_weights(layer, (2, 3), (0,))

        @pl.loop(0, rows // 32)
        def _(i):
            r = pl.ds(pl.multiple_of(i * 32, 32), 32)
            g_in = m.gate[r, :].astype(BF).astype(F32)
            u_in = m.up[r, :].astype(BF).astype(F32)
            h[r, qw:qw + ff] = (g_in * (1.0 / (1.0 + jnp.exp(-g_in))) * u_in).astype(BF)

        rotate(m.qkv, lens, table, groups, head)
        for copy in kv:
            copy.wait()
        attention(m.qkv, lens, m.keys, m.vals, h, (m.lb, m.pb), groups, head, seq)

    def back(layer):
        last = layer == layers - 1
        pair, ici = [], []
        for u, (i, c0, c1) in enumerate(UNITS):
            held = slice(i % 2 * cw + c0, i % 2 * cw + c1)
            pair.append(remote(m.gate.at[:, held], m.recv_p.at[i, :, c0:c1], m.pair_s.at[layer, u], m.pair_r.at[layer, u], mate))
            if i < 3:
                block = pl.ds((i * chunks + c0 // 128) * rows, (c1 - c0) // 128 * rows)
                ici.append(remote(m.keys.at[block], m.recv_i.at[block], m.ici_s.at[layer, u], m.ici_r.at[layer, u],
                                  2 * order[i] + core))

        def settle(u):
            i, c0, c1 = UNITS[u]
            pair[u].wait_recv()
            if i < 3:
                @pl.loop(0, rows // 64)
                def _(n):
                    r = pl.ds(pl.multiple_of(n * 64, 64), 64)
                    for c in range(c0, c1, 128):
                        both = m.up[r, i % 2 * cw + c:i % 2 * cw + c + 128] + m.recv_p[i, r, c:c + 128]
                        to = pl.ds(pl.multiple_of((i * chunks + c // 128) * rows + n * 64, 64), 64)
                        m.keys[to, :] = both.astype(BF)
                ici[u].start()

        for u, (i, c0, c1) in enumerate(UNITS):
            held = i % 2 * cw
            if i >= 2:
                for v in range(n_units):
                    if UNITS[v][0] == i - 2:
                        pair[v].wait_send()
            for which in range(2):
                for copy in out_weights(layer, u, which):
                    copy.wait()
            part = (jnp.dot(h[:, 0:qw], m.wo_w[i % 2, :, 2 * c0:2 * c1], preferred_element_type=F32)
                    + jnp.dot(h[:, qw:qw + ff], down_w(i)[:, 2 * c0:2 * c1], preferred_element_type=F32))
            m.gate[:, held + c0:held + c1] = part[:, 0:c1 - c0]
            pair[u].start()
            m.up[:, held + c0:held + c1] = part[:, c1 - c0:]
            if u == n_units - 1 or UNITS[u + 1][0] != i:
                if i < 2:
                    start_out_weights(layer, (i + 2,), (1,))
                if i % 2 and not last:
                    for copies in in_weights(layer + 1, i // 2, i // 2):
                        start(copies)
            if u >= 1:
                settle(u - 1)
        settle(n_units - 1)
        for copy in ici:
            copy.wait_recv()

        @pl.loop(0, rows // 128)
        def _(n):
            r = pl.ds(pl.multiple_of(n * 128, 128), 128)
            squares = jnp.zeros((128, 128), F32)
            for c in range(chunks):
                cs = pl.ds(pl.multiple_of(me * cw + c * 128, 128), 128)
                total = m.up[r, cw + c * 128:cw + (c + 1) * 128] + m.recv_p[3, r, c * 128:(c + 1) * 128]
                for i in range(3):
                    at = pl.ds(pl.multiple_of((i * chunks + c) * rows + n * 128, 128), 128)
                    total = total + m.recv_i[at, :].astype(F32)
                new = (x[r, cs].astype(F32) + total).astype(BF)
                x[r, cs] = new
                squares = squares + new.astype(F32) * new.astype(F32)
            if not last:
                by_row = jnp.broadcast_to(jnp.sum(squares, axis=-1, keepdims=True), (128, 128))
                m.sums[me, :, r] = by_row.T[0:8]

        gather = gather_plan(me, x, cw, m.ag_s.at[layer], m.ag_r.at[layer])
        near, far, to_mate = gather
        swap_sums = [] if last else [remote(m.sums.at[me], m.sums.at[me], m.sum_s.at[n], m.sum_r.at[n], peer)
                                     for n, peer in enumerate(peers)]
        start(swap_sums + near[:1] + to_mate[:1])
        for copy in ici:
            copy.wait_send()
        for u, (i, _, _) in enumerate(UNITS):
            if i >= 2:
                pair[u].wait_send()
        if not last:
            for n in range(n_peers - 1):
                sender = lax.rem(me + n_peers - 1 - n, n_peers)
                remote(m.sums.at[sender], m.sums.at[sender], m.sum_s.at[n], m.sum_r.at[n], sender).wait_recv()
            for c0 in range(0, rows, 128):
                total = m.sums[0, :, c0:c0 + 128]
                for n in range(1, n_peers):
                    total = total + m.sums[n, :, c0:c0 + 128]
                scale = lax.rsqrt(total / width + NORM_EPS)
                m.inv[c0:c0 + 128, :] = jnp.broadcast_to(scale[0:1], (128, 128)).T
            for copy in swap_sums:
                copy.wait_send()
        return gather

    x_copy = pltpu.make_async_copy(x_hbm, x, m.x_sem)
    x_copy.start()
    early = in_weights(0, 0, 0)
    start(early[0])
    greet(me, peers)
    x_copy.wait()
    start(early[1] + early[2])

    @pl.loop(0, rows // 128)
    def _(i):
        r = pl.ds(pl.multiple_of(i * 128, 128), 128)
        total = jnp.zeros((128, 128), F32)
        for c0 in range(0, width, 128):
            v = x[r, c0:c0 + 128].astype(F32)
            total = total + v * v
        mean = jnp.sum(total, axis=-1, keepdims=True) / width
        m.inv[r, :] = jnp.broadcast_to(lax.rsqrt(mean + NORM_EPS), (128, 128))

    gather = None
    for layer in range(layers):
        front(layer, gather)
        gather = back(layer)

    near, far, to_mate = gather

    def store(n, q):
        block = pl.ds(pl.multiple_of(q * kb, kb), kb)
        return pltpu.make_async_copy(x.at[:, block], out_ref.at[:, block], m.out_sem.at[n])

    out = [store(n, q) for n, q in enumerate((chip, order[2], order[1], order[0]))]
    near[0].wait_send()
    near[1].start()
    for n in range(2):
        near[n].wait_recv()
        far[n].start()
        to_mate[1 + n].start()
    to_mate[0].wait_recv()
    out[0].start()
    for n in range(2):
        far[n].wait_recv()
        to_mate[3 + n].start()
    to_mate[1].wait_recv()
    to_mate[2].wait_recv()
    out[1].start()
    out[2].start()
    to_mate[3].wait_recv()
    to_mate[4].wait_recv()
    out[3].start()
    for copy in near[1:] + far + to_mate:
        copy.wait_send()
    for copy in out:
        copy.wait()


def block_call(layers, rows, width, cw, groups, head, seq, ff):
    hbm = pl.BlockSpec(memory_space=pl.ANY)
    vmem = pl.BlockSpec(memory_space=pltpu.VMEM)
    dma, ram = pltpu.SemaphoreType.DMA, pltpu.VMEM
    qw, kb, n, peers = groups * head, 2 * cw, len(UNITS), width // cw
    joint = (2, PER, groups * 8, 8 * seq + 128)
    return pl.pallas_call(
        functools.partial(block_kernel, (layers, groups, head, seq, cw, width // kb)),
        out_shape=jax.ShapeDtypeStruct((rows, width), BF),
        in_specs=[hbm, vmem, vmem, vmem] + [hbm] * 9,
        out_specs=hbm,
        scratch_shapes=[
            ram((rows, width), BF), ram((rows, kb), BF), ram((rows, 128), F32),
            ram((2, kb, qw + 2 * head), BF), ram((2, ff, kb), BF), ram((2, ff, kb), BF), ram((2, qw, kb), BF),
            ram((rows, qw + 2 * head), F32), ram((rows, ff), F32), ram((rows, ff), F32),
            ram((rows * seq, head), BF), ram((rows * seq, head), BF), ram(joint, F32), ram(joint, F32),
            ram((rows, qw + ff), BF), ram((4, rows, cw), F32), ram((3 * cw // 128 * rows, 128), BF), ram((peers, 8, rows), F32),
            dma, dma((2, 10)), dma((2,)), dma((n, 4)), dma((layers, n)), dma((layers, n)), dma((layers, n)), dma((layers, n)),
            dma((peers - 1,)), dma((peers - 1,)), dma((layers, 9)), dma((layers, 9)), dma((4,)),
        ],
        compiler_params=pltpu.CompilerParams(vmem_limit_bytes=67043328, collective_id=0, has_side_effects=True),
        name="mega",
    )


def solution(mesh):
    tp = mesh.shape["tp"]
    arg_specs = (P("dp", None), P("dp"), P(), P(None, None, "tp"), P(None, None, "tp"), P(None, None, "tp"), P(None, "tp", None), P(None, None, "tp"), P(None, None, "tp"), P(None, "tp", None), P(None, "dp", None, "tp", None), P(None, "dp", None, "tp", None))

    def per_device(x_in, lengths, norm_gain, w_q, w_k, w_v, w_o, w_gate, w_up, w_down, k_cache, v_cache):
        rows, width = x_in.shape
        layers, _, seq, _, head = k_cache.shape
        qw, ff = w_q.shape[-1], w_gate.shape[-1]
        groups = qw // head
        cw = width // tp
        lens = jnp.broadcast_to(lengths.astype(F32)[:, None], (rows, 128))
        table = jnp.asarray(angle_table(seq, head))
        gate_t, up_t = jnp.swapaxes(w_gate, 1, 2), jnp.swapaxes(w_up, 1, 2)
        kc = k_cache.reshape(layers, rows * seq, head)
        vc = v_cache.reshape(layers, rows * seq, head)
        return block_call(layers, rows, width, cw, groups, head, seq, ff)(
            x_in, lens, table, norm_gain, w_q, w_k, w_v, gate_t, up_t, w_o, w_down, kc, vc)

    return jax.shard_map(per_device, mesh=mesh, in_specs=arg_specs, out_specs=P("dp", None), check_vma=False)
```

```python
import functools
import types

import jax
import jax.numpy as jnp
import numpy as np
from jax import lax
from jax.experimental import pallas as pl
from jax.experimental.pallas import tpu as pltpu
from jax.sharding import PartitionSpec as P

NORM_EPS = 1e-5
ROPE_BASE = 500000.0
MESH = pl.DeviceIdType.MESH
BF, F32 = jnp.bfloat16, jnp.float32
PER = 4
LANE = 128
TOK = 8
NT_DIMS = (((1,), (1,)), ((), ()))


def aligned(at, size):
    return pl.ds(pl.multiple_of(at, size), size)


def angle_table(seq, head):
    freq = np.float32(1.0) / np.power(np.float32(ROPE_BASE), np.arange(0, head, 2, dtype=np.float32) / np.float32(head))
    angle = np.arange(seq, dtype=np.float32)[:, None] * freq[None, :]
    cos, sin = np.cos(angle.astype(np.float64)), np.sin(angle.astype(np.float64))
    table = np.zeros((LANE, 2 * head), np.float32)
    table[:seq] = np.concatenate([cos, cos, -sin, sin], axis=1)
    return table


def rotate(qkv, lens, table, groups, head, r0, r1):
    at = lax.broadcasted_iota(jnp.int32, (head, head), 0)
    to = lax.broadcasted_iota(jnp.int32, (head, head), 1)
    swap = (at == lax.rem(to + head // 2, head)).astype(BF)

    @pl.loop(r0 // LANE, r1 // LANE)
    def _(i):
        r = aligned(i * LANE, LANE)
        spot = lax.broadcasted_iota(jnp.int32, (LANE, LANE), 1).astype(F32)
        hot = (lens[r, :] == spot).astype(F32)
        angle = jnp.dot(hot, table[...], precision=lax.Precision.HIGHEST, preferred_element_type=F32)
        c, s = angle[:, 0:head], angle[:, head:2 * head]
        for j in range(groups + 1):
            v = qkv[r, head * j:head * (j + 1)].astype(BF)
            other = jnp.dot(v, swap, preferred_element_type=F32)
            qkv[r, head * j:head * (j + 1)] = v.astype(F32) * c + other * s


def attention(qkv, lens, keys, vals, h_ref, bufs, groups, head, seq, r0, r1):
    lb, pb = bufs
    per = lb.shape[0]
    span = TOK * seq
    g0, g1 = r0 // (TOK * per), r1 // (TOK * per)
    scale = head ** -0.5
    col = lax.broadcasted_iota(jnp.int32, (TOK, span), 1).astype(F32)
    low = (lax.broadcasted_iota(jnp.int32, (TOK, span), 0) * seq).astype(F32)
    own = lax.broadcasted_iota(jnp.int32, (TOK, LANE), 0) == lax.broadcasted_iota(jnp.int32, (TOK, LANE), 1)
    none = jnp.zeros((120, head), BF)

    def block(g, n):
        t0 = pl.multiple_of(g * (TOK * per) + 8 * n, 8)
        return t0, pl.ds(t0, 8), pl.ds(pl.multiple_of(t0 * seq, span), span)

    def score(g):
        for n in range(per):
            t0, rows, cached = block(g, n)
            q = jnp.concatenate([qkv[rows, head * j:head * (j + 1)] for j in range(groups)], axis=0).astype(BF)
            k_new = jnp.concatenate([qkv[rows, groups * head:(groups + 1) * head].astype(BF), none], axis=0)
            old = lax.dot_general(q, keys[cached, :], NT_DIMS, preferred_element_type=F32) * scale
            new = lax.dot_general(q, k_new, NT_DIMS, preferred_element_type=F32) * scale
            high = jnp.concatenate([lens[rows, :]] * (span // LANE), axis=1) + low
            keep = (col >= low) & (col < high)
            for j in range(groups):
                r = slice(TOK * j, TOK * (j + 1))
                lb[n, r, 0:span] = jnp.where(keep, old[r], -jnp.inf)
                lb[n, r, span:] = jnp.where(own, new[r], -jnp.inf)

    def weigh(_):
        for n in range(per):
            for j in range(groups):
                r = slice(TOK * j, TOK * (j + 1))
                logits = [lb[n, r, c0:c0 + LANE] for c0 in range(0, span + LANE, LANE)]
                peak = jnp.max(functools.reduce(jnp.maximum, logits), axis=-1, keepdims=True)
                w = [jnp.exp(v - peak) for v in logits]
                inv = 1.0 / jnp.sum(functools.reduce(jnp.add, w), axis=-1, keepdims=True)
                for m, v in enumerate(w):
                    pb[n, r, LANE * m:LANE * (m + 1)] = v * inv

    def mix(g):
        for n0 in range(0, per, 2):
            outs = []
            for n in (n0, n0 + 1):
                t0, rows, cached = block(g, n)
                p = pb[n].astype(BF)
                v_new = jnp.concatenate([qkv[rows, (groups + 1) * head:].astype(BF), none], axis=0)
                outs.append(jnp.dot(p[:, 0:span], vals[cached, :], preferred_element_type=F32)
                            + jnp.dot(p[:, span:], v_new, preferred_element_type=F32))
            rows = pl.ds(pl.multiple_of(block(g, n0)[0], 16), 16)
            for j in range(groups):
                both = jnp.concatenate([o[TOK * j:TOK * (j + 1)] for o in outs], axis=0).astype(BF)
                h_ref[rows, head * j:head * (j + 1)] = both

    @pl.loop(g0, g1 + 2)
    def _(i):
        for lag, stage in ((2, mix), (1, weigh), (0, score)):
            stage(jnp.clip(i - lag, g0, g1 - 1))


def place(core, chip, fx, fy):
    x, y = lax.rem(chip, 2), chip // 2
    return 2 * (y + fy * (1 - 2 * y)) + (x + fx * (1 - 2 * x))


def remote(src, dst, send_sem, recv_sem, device):
    return pltpu.make_async_remote_copy(src_ref=src, dst_ref=dst, send_sem=send_sem, recv_sem=recv_sem,
                                        device_id={"tp": device}, device_id_type=MESH)


def columns(device, width):
    return pl.ds(pl.multiple_of(device * width, width), width)


def gather_plan(me, xg, cw, send_sem, recv_sem):
    core, chip = lax.rem(me, 2), me // 2
    mate = me + 1 - 2 * core
    first = 2 * place(core, chip, 1 - core, core) + core
    second = 2 * place(core, chip, core, 1 - core) + core
    across = 2 * (3 - chip) + core
    rows = xg.shape[0]
    half = rows // 2

    def share(n, r0, r1, owner, device):
        block = xg.at[r0:r1, columns(owner, cw)]
        return remote(block, block, send_sem.at[n], recv_sem.at[n], device)

    near = [share(0, 0, rows, me, first), share(1, 0, rows, me, second)]
    far = [share(2, 0, half, first, second), share(3, half, rows, second, first)]
    to_mate = [share(4, 0, rows, me, mate), share(5, 0, rows, first, mate), share(6, 0, rows, second, mate),
               share(7, 0, half, across, mate), share(8, half, rows, across, mate)]
    return near, far, to_mate


def greet(me, peers):
    barrier = pltpu.get_barrier_semaphore()
    for device in peers:
        pl.semaphore_signal(barrier, inc=1, device_id={"tp": device}, device_id_type=MESH)
    pl.semaphore_wait(barrier, len(peers))


UNITS = ((0, 0, 256, 0, 0), (0, 256, 640, 0, 0), (1, 0, 640, 0, 0), (2, 0, 640, 0, 0),
         (0, 0, 640, 1, 1), (1, 0, 640, 1, 1), (2, 0, 640, 1, 1), (3, 0, 640, 0, 1))
EARLY = 4
PIECES = ((0, 0, 256), (0, 256, 640), (1, 0, 640), (2, 0, 640), (3, 0, 640))
SCRATCH = ("x", "a", "inv", "qkv_w", "twin_w", "wo_w", "qkv", "twin", "keys", "vals", "lb", "pb", "h", "recv_p",
           "recv_i", "sums", "x_sem", "w_sem", "kv_sem", "out_w_sem", "pair_s", "pair_r", "ici_s", "ici_r", "sum_s", "sum_r",
           "ag_s", "ag_r", "out_sem")


def block_kernel(dims, x_hbm, lens, table, gain, wq, wk, wv, wg, wu, wo, wd, kc, vc, out_ref, *scratch):
    layers, groups, head, seq, cw, steps = dims
    m = types.SimpleNamespace(**dict(zip(SCRATCH, scratch, strict=True)))
    m.gate_w, m.up_w, m.gate, m.up = m.twin_w.at[0], m.twin_w.at[1], m.twin.at[0], m.twin.at[1]
    x, h = m.x, m.h
    rows, width = x.shape
    qw, ff, kb = groups * head, m.twin.shape[2], 2 * cw
    n_units, n_peers = len(UNITS), width // cw
    me = lax.axis_index("tp")
    core, chip = lax.rem(me, 2), me // 2
    mate = me + 1 - 2 * core
    order = (place(core, chip, 1, 1), place(core, chip, 0, 1), place(core, chip, 1, 0), chip)
    peers = [lax.rem(me + n, n_peers) for n in range(1, n_peers)]
    chunks, half = cw // LANE, rows // 2

    def start(copies):
        for copy in copies:
            copy.start()

    def sources(step):
        moved, both = (step + 2) // 3, step // 3
        swap = step // 2 * (1 - lax.rem(step, 2))
        return 2 * place(core, chip, moved, both) + swap, 2 * place(core, chip, both, moved) + 1 - swap

    def in_weights(layer, step, slot):
        found = ([], [], [])
        for part, device in enumerate(sources(step)):
            ks, to = columns(device, cw), slice(part * cw, (part + 1) * cw)
            pairs = (
                (0, wq.at[layer, ks, :], m.qkv_w.at[slot, to, 0:qw]),
                (0, wk.at[layer, ks, :], m.qkv_w.at[slot, to, qw:qw + head]),
                (0, wv.at[layer, ks, :], m.qkv_w.at[slot, to, qw + head:qw + 2 * head]),
                (1, wg.at[layer, :, ks], m.gate_w.at[slot, :, to]),
                (2, wu.at[layer, :, ks], m.up_w.at[slot, :, to]),
            )
            for n, (which, src, dst) in enumerate(pairs):
                found[which].append(pltpu.make_async_copy(src, dst, m.w_sem.at[slot, part * 5 + n]))
        return found

    def down_w(i):
        return (m.gate_w, m.up_w)[i % 2].at[i // 2]

    def out_weights(layer, u, which):
        i, c0, c1 = PIECES[u]
        copies = []
        for n, device in enumerate((2 * order[i] + 1 - core, 2 * order[i] + core)):
            at = 2 * c0 + n * (c1 - c0)
            src, dst = ((wd, down_w(i)), (wo, m.wo_w.at[i % 3]))[which]
            copies.append(pltpu.make_async_copy(
                src.at[layer, :, pl.ds(pl.multiple_of(device * cw + c0, LANE), c1 - c0)],
                dst.at[:, at:at + c1 - c0], m.out_w_sem.at[u, 2 * which + n]))
        return copies

    def start_out_weights(layer, tiles, whiches):
        for u, (i, _, _) in enumerate(PIECES):
            if i in tiles:
                for which in whiches:
                    start(out_weights(layer, u, which))

    def cache(layer):
        return [pltpu.make_async_copy(kc.at[layer], m.keys, m.kv_sem.at[0]),
                pltpu.make_async_copy(vc.at[layer], m.vals, m.kv_sem.at[1])]

    def front(layer, gather):
        kv = cache(layer)
        if gather:
            near, far, to_mate = gather

        @pl.loop(0, steps)
        def _(step):
            slot = lax.rem(step, 2)
            if gather:
                for n in range(3):
                    @pl.when(step == n)
                    def _(n=n):
                        to_mate[n].wait_recv()

                @pl.when(step == 3)
                def _():
                    to_mate[3].wait_recv()
                    to_mate[4].wait_recv()

            devices = sources(step)

            @pl.loop(0, rows // 64)
            def _(i):
                r = aligned(i * 64, 64)
                inv = m.inv[r, :]
                for part, device in enumerate(devices):
                    for c0 in range(0, cw, LANE):
                        cs = aligned(device * cw + c0, LANE)
                        g = gain[layer:layer + 1, cs].astype(F32)
                        m.a[r, part * cw + c0:part * cw + c0 + LANE] = (x[r, cs].astype(F32) * inv * g).astype(BF)

            first = step == 0
            w_copies = in_weights(layer, step, slot)
            for copy in w_copies[0]:
                copy.wait()
            part = jnp.dot(m.a[...], m.qkv_w[slot], preferred_element_type=F32)
            m.qkv[...] = jnp.where(first, 0.0, m.qkv[...]) + part

            @pl.loop(0, 2)
            def _(which):
                for n in range(2):
                    @pl.when(which == n)
                    def _(n=n):
                        for copy in w_copies[1 + n]:
                            copy.wait()

                def at(k, n):
                    return jnp.logical_and(step == k, which == n)

                if not gather:
                    @pl.when(at(0, 0))
                    def _():
                        for copies in in_weights(layer, 1, 1):
                            start(copies)

                part = lax.dot_general(m.a[...], m.twin_w[which, slot], NT_DIMS, preferred_element_type=F32)
                m.twin[which] = jnp.where(first, 0.0, m.twin[which]) + part
                if gather:
                    @pl.when(at(0, 0))
                    def _():
                        near[0].wait_send()
                        near[1].start()
                        near[0].wait_recv()
                        to_mate[1].start()
                        far[0].start()

                    @pl.when(at(1, 1))
                    def _():
                        near[1].wait_recv()
                        to_mate[2].start()
                        far[1].start()

                    @pl.when(at(2, 1))
                    def _():
                        far[0].wait_recv()
                        to_mate[3].start()
                        far[1].wait_recv()
                        to_mate[4].start()

            @pl.when(step + 2 < steps)
            def _():
                for copies in in_weights(layer, step + 2, slot):
                    start(copies)

            @pl.when(step == 1)
            def _():
                start(kv)

            @pl.when(step == 2)
            def _():
                start_out_weights(layer, (0, 1), (0,))
                start_out_weights(layer, (0, 1, 2), (1,))

        if gather:
            for copy in near[1:] + far + to_mate:
                copy.wait_send()
        start_out_weights(layer, (2, 3), (0,))

    def gate_rows(r0, r1):
        @pl.loop(r0 // 32, r1 // 32)
        def _(i):
            r = aligned(i * 32, 32)
            g_in = m.gate[r, :].astype(BF).astype(F32)
            u_in = m.up[r, :].astype(BF).astype(F32)
            h[r, qw:qw + ff] = (g_in * (1.0 / (1.0 + jnp.exp(-g_in))) * u_in).astype(BF)

        rotate(m.qkv, lens, table, groups, head, r0, r1)

    def back(layer):
        last = layer == layers - 1
        pair, ici = [], []
        for u, (i, c0, c1, h0, h1) in enumerate(UNITS):
            held, r = slice(i % 2 * cw + c0, i % 2 * cw + c1), slice(h0 * half, (h1 + 1) * half)
            pair.append(remote(m.gate.at[r, held], m.recv_p.at[i % 3, r, c0:c1], m.pair_s.at[layer, u], m.pair_r.at[layer, u], mate))
            if i < 3:
                block = pl.ds(((2 * i + h0) * chunks + c0 // LANE) * half, (c1 - c0) // LANE * half)
                ici.append(remote(m.keys.at[block], m.recv_i.at[block], m.ici_s.at[layer, u], m.ici_r.at[layer, u],
                                  2 * order[i] + core))

        def settle(u):
            i, c0, c1, h0, _ = UNITS[u]
            pair[u].wait_recv()
            if i < 3:
                @pl.loop(0, half // 64)
                def _(n):
                    r = pl.ds(pl.multiple_of(h0 * half + n * 64, 64), 64)
                    for c in range(c0, c1, LANE):
                        both = m.up[r, i % 2 * cw + c:i % 2 * cw + c + LANE] + m.recv_p[i % 3, r, c:c + LANE]
                        to = pl.ds(pl.multiple_of(((2 * i + h0) * chunks + c // LANE) * half + n * 64, 64), 64)
                        m.keys[to, :] = both.astype(BF)
                ici[u].start()

        def attend(r0, r1):
            attention(m.qkv, lens, m.keys, m.vals, h, (m.lb, m.pb), groups, head, seq, r0, r1)

        gate_rows(0, half)
        for copy in cache(layer):
            copy.wait()
        attend(0, half)
        sent = set()
        loaded = set()
        for u, (i, c0, c1, h0, h1) in enumerate(UNITS):
            held, r = i % 2 * cw, slice(h0 * half, (h1 + 1) * half)
            if u == EARLY:
                gate_rows(half, rows)
                settle(u - 1)
                attend(half, rows)
            for v in range(u):
                if v not in sent and UNITS[v][0] % 2 == i % 2 and UNITS[v][0] != i and UNITS[v][3] <= h1 and UNITS[v][4] >= h0:
                    pair[v].wait_send()
                    sent.add(v)
            for p, (t, p0, p1) in enumerate(PIECES):
                if t == i and p0 < c1 and p1 > c0 and p not in loaded:
                    loaded.add(p)
                    for which in range(2):
                        for copy in out_weights(layer, p, which):
                            copy.wait()
            inner = [(p0, p1) for t, p0, p1 in PIECES if t == i and p0 < c1 and p1 > c0]
            for p0, p1 in inner:
                part = (jnp.dot(h[r, 0:qw], m.wo_w[i % 3, :, 2 * p0:2 * p1], preferred_element_type=F32)
                        + jnp.dot(h[r, qw:qw + ff], down_w(i)[:, 2 * p0:2 * p1], preferred_element_type=F32))
                m.gate[r, held + p0:held + p1] = part[:, 0:p1 - p0]
                m.up[r, held + p0:held + p1] = part[:, p1 - p0:]
            if u == n_units - 1:
                settle(u - 1)
            pair[u].start()
            if u == EARLY:
                start_out_weights(layer, (3,), (1,))
            if not last and u in (n_units - 3, n_units - 1):
                for copies in in_weights(layer + 1, u // (n_units - 1), u // (n_units - 1)):
                    start(copies)
            if u >= 1 and u not in (EARLY, n_units - 1):
                settle(u - 1)
        settle(n_units - 1)
        for copy in ici:
            copy.wait_recv()

        @pl.loop(0, rows // LANE)
        def _(n):
            r = aligned(n * LANE, LANE)
            squares = jnp.zeros((LANE, LANE), F32)
            for c in range(chunks):
                cs = aligned(me * cw + c * LANE, LANE)
                total = m.up[r, cw + c * LANE:cw + (c + 1) * LANE] + m.recv_p[0, r, c * LANE:(c + 1) * LANE]
                for i in range(3):
                    at = ((2 * i + n // (half // LANE)) * chunks + c) * half + lax.rem(n, half // LANE) * LANE
                    at = aligned(at, LANE)
                    total = total + m.recv_i[at, :].astype(F32)
                new = (x[r, cs].astype(F32) + total).astype(BF)
                x[r, cs] = new
                squares = squares + new.astype(F32) * new.astype(F32)
            if not last:
                by_row = jnp.broadcast_to(jnp.sum(squares, axis=-1, keepdims=True), (LANE, LANE))
                m.sums[me, :, r] = by_row.T[0:8]

        gather = gather_plan(me, x, cw, m.ag_s.at[layer], m.ag_r.at[layer])
        near, far, to_mate = gather
        swap_sums = [] if last else [remote(m.sums.at[me], m.sums.at[me], m.sum_s.at[n], m.sum_r.at[n], peer)
                                     for n, peer in enumerate(peers)]
        start(swap_sums + near[:1] + to_mate[:1])
        for copy in ici:
            copy.wait_send()
        for u in range(n_units):
            if u not in sent:
                pair[u].wait_send()
        if not last:
            for n in range(n_peers - 1):
                sender = lax.rem(me + n_peers - 1 - n, n_peers)
                remote(m.sums.at[sender], m.sums.at[sender], m.sum_s.at[n], m.sum_r.at[n], sender).wait_recv()
            for c0 in range(0, rows, LANE):
                total = m.sums[0, :, c0:c0 + LANE]
                for n in range(1, n_peers):
                    total = total + m.sums[n, :, c0:c0 + LANE]
                scale = lax.rsqrt(total / width + NORM_EPS)
                m.inv[c0:c0 + LANE, :] = jnp.broadcast_to(scale[0:1], (LANE, LANE)).T
            for copy in swap_sums:
                copy.wait_send()
        return gather

    x_copy = pltpu.make_async_copy(x_hbm, x, m.x_sem)
    x_copy.start()
    early = in_weights(0, 0, 0)
    start(early[0])
    greet(me, peers)
    x_copy.wait()
    start(early[1] + early[2])

    @pl.loop(0, rows // LANE)
    def _(i):
        r = aligned(i * LANE, LANE)
        total = jnp.zeros((LANE, LANE), F32)
        for c0 in range(0, width, LANE):
            v = x[r, c0:c0 + LANE].astype(F32)
            total = total + v * v
        mean = jnp.sum(total, axis=-1, keepdims=True) / width
        m.inv[r, :] = jnp.broadcast_to(lax.rsqrt(mean + NORM_EPS), (LANE, LANE))

    gather = None
    for layer in range(layers):
        front(layer, gather)
        gather = back(layer)

    near, far, to_mate = gather

    def store(n, q):
        block = pl.ds(pl.multiple_of(q * kb, kb), kb)
        return pltpu.make_async_copy(x.at[:, block], out_ref.at[:, block], m.out_sem.at[n])

    out = [store(n, q) for n, q in enumerate((chip, order[2], order[1], order[0]))]
    near[0].wait_send()
    near[1].start()
    for n in range(2):
        near[n].wait_recv()
        far[n].start()
        to_mate[1 + n].start()
    to_mate[0].wait_recv()
    out[0].start()
    for n in range(2):
        far[n].wait_recv()
        to_mate[3 + n].start()
    to_mate[1].wait_recv()
    to_mate[2].wait_recv()
    out[1].start()
    out[2].start()
    to_mate[3].wait_recv()
    to_mate[4].wait_recv()
    out[3].start()
    for copy in near[1:] + far + to_mate:
        copy.wait_send()
    for copy in out:
        copy.wait()


def block_call(layers, rows, width, cw, groups, head, seq, ff):
    hbm = pl.BlockSpec(memory_space=pl.ANY)
    vmem = pl.BlockSpec(memory_space=pltpu.VMEM)
    dma, ram = pltpu.SemaphoreType.DMA, pltpu.VMEM
    qw, kb, n, peers = groups * head, 2 * cw, len(UNITS), width // cw
    joint = (PER, groups * 8, TOK * seq + LANE)
    return pl.pallas_call(
        functools.partial(block_kernel, (layers, groups, head, seq, cw, width // kb)),
        out_shape=jax.ShapeDtypeStruct((rows, width), BF),
        in_specs=[hbm, vmem, vmem, vmem] + [hbm] * 9,
        out_specs=hbm,
        scratch_shapes=[
            ram((rows, width), BF), ram((rows, kb), BF), ram((rows, LANE), F32),
            ram((2, kb, qw + 2 * head), BF), ram((2, 2, ff, kb), BF), ram((3, qw, kb), BF),
            ram((rows, qw + 2 * head), F32), ram((2, rows, ff), F32),
            ram((rows * seq, head), BF), ram((rows * seq, head), BF), ram(joint, F32), ram(joint, F32),
            ram((rows, qw + ff), BF), ram((3, rows, cw), F32), ram((3 * cw // LANE * rows, LANE), BF), ram((peers, 8, rows), F32),
            dma, dma((2, 10)), dma((2,)), dma((len(PIECES), 4)), dma((layers, n)), dma((layers, n)), dma((layers, n)), dma((layers, n)),
            dma((peers - 1,)), dma((peers - 1,)), dma((layers, 9)), dma((layers, 9)), dma((4,)),
        ],
        compiler_params=pltpu.CompilerParams(vmem_limit_bytes=67043328, collective_id=0, has_side_effects=True),
        name="mega",
    )


def solution(mesh):
    tp = mesh.shape["tp"]
    arg_specs = (P("dp", None), P("dp"), P(), P(None, None, "tp"), P(None, None, "tp"), P(None, None, "tp"), P(None, "tp", None), P(None, None, "tp"), P(None, None, "tp"), P(None, "tp", None), P(None, "dp", None, "tp", None), P(None, "dp", None, "tp", None))

    def per_device(x_in, lengths, norm_gain, w_q, w_k, w_v, w_o, w_gate, w_up, w_down, k_cache, v_cache):
        rows, width = x_in.shape
        layers, _, seq, _, head = k_cache.shape
        qw, ff = w_q.shape[-1], w_gate.shape[-1]
        groups = qw // head
        cw = width // tp
        lens = jnp.broadcast_to(lengths.astype(F32)[:, None], (rows, LANE))
        table = jnp.asarray(angle_table(seq, head))
        gate_t, up_t = jnp.swapaxes(w_gate, 1, 2), jnp.swapaxes(w_up, 1, 2)
        kc = k_cache.reshape(layers, rows * seq, head)
        vc = v_cache.reshape(layers, rows * seq, head)
        return block_call(layers, rows, width, cw, groups, head, seq, ff)(
            x_in, lens, table, norm_gain, w_q, w_k, w_v, gate_t, up_t, w_o, w_down, kc, vc)

    return jax.shard_map(per_device, mesh=mesh, in_specs=arg_specs, out_specs=P("dp", None), check_vma=False)
```
